32 devices in a mesh: rhs: 1 (over z), mz: 4 (over y), my: 4 (over x), mx: 2 (over core).
Axes of the slice: x: 4, y: 4, z: 1, core: 2. Of those that a mesh axis runs over, the one named last changes fastest.
The devices are a block of a 4x4x8 slice.
Arguments:
- x_vol: bfloat16 [512, 512, 512, 1], P('mx', 'my', 'mz', 'rhs')
- fac_a1: bfloat16 [128, 512], replicated
- fac_a2: bfloat16 [128, 512], replicated
- fac_a3: bfloat16 [128, 512], replicated
- diag_d: float32 [128, 128, 128], P('mx', 'my', 'mz')
- fac_b1: bfloat16 [512, 128], replicated
- fac_b2: bfloat16 [512, 128], replicated
- fac_b3: bfloat16 [512, 128], replicated
Outputs:
- output: float32 [512, 512, 512, 1], P('mx', 'my', 'mz', 'rhs')
All inputs are finite; a program needn't handle non-finite values.
Results may differ from the reference program's by a relative error of at most 0.0126989.
Values are sent between devices in bfloat16 or wider.
A program may use at most 768 MiB of HBM per device.

```python
import jax
import jax.numpy as jnp

N1 = 512
N2 = 512
N3 = 512
C = 1
M1 = N1 // 4
M2 = N2 // 4
M3 = N3 // 4


def setup_inputs(seed: int = 0, part: int = 0) -> dict:
    base_key = jax.random.key(seed)
    key_list = jax.random.split(base_key, 8)
    vol_key = jax.random.fold_in(key_list[0], part)
    x_vol = jax.random.normal(vol_key, (N1, N2, N3, C), jnp.float32).astype(jnp.bfloat16)
    fac_a1 = (jax.random.normal(key_list[1], (M1, N1), jnp.float32) * N1 ** -0.5).astype(jnp.bfloat16)
    fac_a2 = (jax.random.normal(key_list[2], (M2, N2), jnp.float32) * N2 ** -0.5).astype(jnp.bfloat16)
    fac_a3 = (jax.random.normal(key_list[3], (M3, N3), jnp.float32) * N3 ** -0.5).astype(jnp.bfloat16)
    diag_d = jnp.exp(jax.random.uniform(key_list[4], (M1, M2, M3), jnp.float32, -1.15, 1.15))
    fac_b1 = (jax.random.normal(key_list[5], (N1, M1), jnp.float32) * M1 ** -0.5).astype(jnp.bfloat16)
    fac_b2 = (jax.random.normal(key_list[6], (N2, M2), jnp.float32) * M2 ** -0.5).astype(jnp.bfloat16)
    fac_b3 = (jax.random.normal(key_list[7], (N3, M3), jnp.float32) * M3 ** -0.5).astype(jnp.bfloat16)
    return {"x_vol": x_vol, "fac_a1": fac_a1, "fac_a2": fac_a2, "fac_a3": fac_a3, "diag_d": diag_d, "fac_b1": fac_b1, "fac_b2": fac_b2, "fac_b3": fac_b3}


def mode_product(matrix, tensor, form):
    return jnp.einsum(form, matrix.astype(jnp.float32), tensor.astype(jnp.float32))


def reference(x_vol, fac_a1, fac_a2, fac_a3, diag_d, fac_b1, fac_b2, fac_b3):
    u_one = mode_product(fac_a1, x_vol, "ia,ajkr->ijkr").astype(jnp.bfloat16)
    u_two = mode_product(fac_a2, u_one, "jb,ibkr->ijkr").astype(jnp.bfloat16)
    u_three = mode_product(fac_a3, u_two, "kc,ijcr->ijkr").astype(jnp.bfloat16)
    w_core = (diag_d[:, :, :, None] * u_three.astype(jnp.float32)).astype(jnp.bfloat16)
    v_three = mode_product(fac_b3, w_core, "kc,ijcr->ijkr").astype(jnp.bfloat16)
    v_two = mode_product(fac_b2, v_three, "jb,ibkr->ijkr").astype(jnp.bfloat16)
    return mode_product(fac_b1, v_two, "ia,ajkr->ijkr")
```

```python
import functools

import jax
import jax.numpy as jnp
from jax import lax
from jax.experimental import pallas as pl
from jax.experimental.pallas import tpu as pltpu
from jax.sharding import PartitionSpec as P

MESH = pl.DeviceIdType.MESH
F32 = jnp.float32
BF16 = jnp.bfloat16
CHUNK = 16
NT = (((1,), (1,)), ((), ()))


def core_kernel(sizes, x_hbm, a1_ref, a2_ref, a3_ref, d_ref, b2_ref, b3_ref, v2_hbm,
                xb, xs, uf, u1, u1r, u2, u2r, dsend, dmid, drecv, dfull, wg, v2s,
                sem_lx, sem_x, sem_d1, sem_d2, sem_u1, sem_u2, sem_w0, sem_w1, sem_v, sem_lv):
    n_m, n_x, n_y, groups = sizes
    m, xx, yy = lax.axis_index("mx"), lax.axis_index("my"), lax.axis_index("mz")
    rows_a = x_hbm.shape[0]
    half = x_hbm.shape[1] // n_m
    n_chunk = half // CHUNK
    m1 = a1_ref.shape[0]
    ib = m1 // (n_m * n_x)
    ig = ib // groups
    jb = u2r.shape[2]
    im = ib * n_x

    def shift(dm=0, dx=0, dy=0):
        return {"mx": lax.rem(m + dm, n_m), "my": lax.rem(xx + dx, n_x), "mz": lax.rem(yy + dy, n_y)}

    def remote(src, dst, sems, idx, dev):
        return pltpu.make_async_remote_copy(
            src_ref=src, dst_ref=dst, send_sem=sems.at[(0,) + idx], recv_sem=sems.at[(1,) + idx],
            device_id=dev, device_id_type=MESH)

    row = [(dm, dx) for dx in range(n_x) for dm in range(n_m) if (dm, dx) != (0, 0)]

    loads = []
    for q in range(n_chunk):
        cp = pltpu.make_async_copy(
            x_hbm.at[:, pl.ds(m * half + q * CHUNK, CHUNK), :], xb.at[q, m], sem_lx.at[q])
        cp.start()
        loads.append(cp)
    barrier = pltpu.get_barrier_semaphore()
    for dm, dx in row:
        pl.semaphore_signal(barrier, inc=1, device_id=shift(dm, dx), device_id_type=MESH)
    for dy in range(1, n_y):
        pl.semaphore_signal(barrier, inc=1, device_id=shift(dy=dy), device_id_type=MESH)

    dsend[...] = jnp.swapaxes(d_ref[...], 1, 2)
    pl.semaphore_wait(barrier, len(row) + n_y - 1)

    x_cp = []
    for q in range(n_chunk):
        cp = remote(x_hbm.at[:, pl.ds((1 - m) * half + q * CHUNK, CHUNK), :], xb.at[q, m], sem_x, (q,), shift(dm=1))
        cp.start()
        x_cp.append(cp)
    d1_cp = []
    for dx in range(1, n_x):
        to = lax.rem(xx + dx, n_x)
        cp = remote(dsend.at[:, pl.ds(to * ib, ib), :], dmid.at[xx], sem_d1, (dx - 1,), shift(dx=dx))
        cp.start()
        d1_cp.append(cp)
    dmid[xx] = dsend[:, pl.ds(pl.multiple_of(xx * ib, ib), ib), :]

    me = xx * n_m + m
    u1_cp = [[] for _ in range(groups)]

    def send_u1(q, g):
        for r, (dm, dx) in enumerate(row):
            base = lax.rem(m + dm, n_m) * im + lax.rem(xx + dx, n_x) * ib + g * ig
            cp = remote(u1.at[q, pl.ds(base, ig)], u1r.at[me, q, pl.ds(g * ig, ig)],
                        sem_u1, (q, g, r), shift(dm, dx))
            cp.start()
            u1_cp[g].append(cp)

    step = m1 // 4
    for q in range(n_chunk):
        loads[q].wait()
        x_cp[q].wait_recv()
        for s in range(n_m):
            @pl.loop(0, rows_a // 128)
            def _(c, s=s, q=q):
                v = xb[q, s, pl.ds(c * 128, 128)].astype(F32)
                xs[:, pl.ds(s * rows_a + c * 128, 128), :] = jnp.swapaxes(v, 0, 1).astype(BF16)

        @pl.loop(0, CHUNK // 2)
        def _(b):
            rhs = jnp.concatenate([xs[2 * b], xs[2 * b + 1]], axis=1)
            out = jnp.dot(a1_ref[...], rhs, preferred_element_type=F32)
            lanes = out.shape[1] // 2
            uf[2 * b] = out[:, :lanes]
            uf[2 * b + 1] = out[:, lanes:]

        @pl.loop(0, 4)
        def _(c, q=q):
            v = uf[:, pl.ds(pl.multiple_of(c * step, step), step), :]
            u1[q, pl.ds(c * step, step)] = jnp.swapaxes(v, 0, 1).astype(BF16)

        u1r[me, q] = u1[q, pl.ds(m * im + xx * ib, ib)]
        send_u1(q, 0)
        if q == 0:
            d2_cp = []
            for cp in d1_cp:
                cp.wait_recv()
            for dy in range(1, n_y):
                to = lax.rem(yy + dy, n_y)
                cp = remote(dmid.at[to], drecv.at[yy], sem_d2, (dy - 1,), shift(dy=dy))
                cp.start()
                d2_cp.append(cp)
            drecv[yy] = dmid[yy]
    for g in range(1, groups):
        for q in range(n_chunk):
            send_u1(q, g)
    for cp in d2_cp:
        cp.wait_recv()
    dfull[...] = jnp.swapaxes(jnp.concatenate([drecv[s] for s in range(n_y)], axis=2), 0, 1)

    u2_cp = [[] for _ in range(groups)]

    def mode2(g):
        for cp in u1_cp[g]:
            cp.wait_recv()

        @pl.loop(0, ig // 2)
        def _(t):
            i = g * ig + 2 * t
            parts = [u1r[:, :, i + h].reshape(-1, u1r.shape[-1]) for h in range(2)]
            out = jnp.dot(a2_ref[...], jnp.concatenate(parts, axis=1), preferred_element_type=F32)
            lanes = out.shape[1] // 2
            u2[i] = out[:, :lanes].astype(BF16)
            u2[i + 1] = out[:, lanes:].astype(BF16)

        isl = pl.ds(g * ig, ig)
        for dy in range(1, n_y):
            to = lax.rem(yy + dy, n_y)
            cp = remote(u2.at[isl, pl.ds(to * jb, jb), :], u2r.at[yy, isl], sem_u2, (g, dy - 1), shift(dy=dy))
            cp.start()
            u2_cp[g].append(cp)
        u2r[yy, isl] = u2[isl, pl.ds(pl.multiple_of(yy * jb, jb), jb), :]

    def mode3(g):
        for cp in u2_cp[g]:
            cp.wait_recv()
        isl = pl.ds(g * ig, ig)
        parts = [u2r[s, isl].reshape(ig * jb, -1) for s in range(n_y)]
        out = lax.dot_general(jnp.concatenate(parts, axis=1), a3_ref[...], NT, preferred_element_type=F32)
        u3 = out.astype(BF16).astype(F32).reshape(ig, jb, -1)
        wg[xx, isl, pl.ds(pl.multiple_of(yy * jb, jb), jb), :] = (dfull[isl] * u3).astype(BF16)

    for g in range(groups):
        mode2(g)
        mode3(g)

    h = ib // 2
    h0, h1 = pl.ds(0, h), pl.ds(h, h)
    jy = pl.ds(pl.multiple_of(yy * jb, jb), jb)
    w0a, w1a, w0b, w1b = [], [], [], []
    for dy in range(1, n_y):
        ref = wg.at[xx, h0, jy, :]
        w0a.append(remote(ref, ref, sem_w0, (0, dy - 1), shift(dy=dy)))
        w0a[-1].start()
    for dx in range(1, n_x):
        ref = wg.at[xx, h1, jy, :]
        w1a.append(remote(ref, ref, sem_w1, (0, dx - 1), shift(dx=dx)))
        w1a[-1].start()
    for cp in w0a:
        cp.wait_recv()
    for dx in range(1, n_x):
        ref = wg.at[xx, h0]
        w0b.append(remote(ref, ref, sem_w0, (1, dx - 1), shift(dx=dx)))
        w0b[-1].start()
    for cp in w1a:
        cp.wait_recv()
    for dy in range(1, n_y):
        ref = wg.at[:, h1, jy, :]
        w1b.append(remote(ref, ref, sem_w1, (1, dy - 1), shift(dy=dy)))
        w1b[-1].start()
    for cp in w0b:
        cp.wait_recv()
    for cp in w1b:
        cp.wait_recv()

    b3 = b3_ref[pl.ds(pl.multiple_of(yy * b3_ref.shape[1], 128), v2s.shape[2]), :]
    nj = v2s.shape[1]
    b2 = b2_ref[pl.ds(pl.multiple_of(xx * b2_ref.shape[1], 128), nj), :]
    v_cp = []
    for s in range(n_x):
        @pl.loop(0, ib // 2)
        def _(t, s=s):
            w = wg[s, pl.ds(2 * t, 2)].reshape(2 * wg.shape[2], -1)
            v3 = lax.dot_general(w, b3, NT, preferred_element_type=F32).astype(BF16)
            rows = v3.shape[0] // 2
            rhs = jnp.concatenate([v3[:rows], v3[rows:]], axis=1)
            out = jnp.dot(b2, rhs, preferred_element_type=F32).astype(BF16)
            lanes = out.shape[1] // 2
            v2s[s * ib + 2 * t] = out[:, :lanes]
            v2s[s * ib + 2 * t + 1] = out[:, lanes:]

        src = v2s.at[pl.ds(s * ib, ib)]
        dst = v2_hbm.at[pl.ds(m * im + s * ib, ib)]
        cp = remote(src, dst, sem_v, (s,), shift(dm=1))
        cp.start()
        v_cp.append(cp)
        lcp = pltpu.make_async_copy(src, dst, sem_lv.at[s])
        lcp.start()
        loads.append(lcp)
    for cp in loads[n_chunk:]:
        cp.wait()
    for cp in v_cp:
        cp.wait_recv()
    for cp in x_cp + d1_cp + d2_cp + sum(u1_cp, []) + sum(u2_cp, []) + w0a + w0b + w1a + w1b + v_cp:
        cp.wait_send()


def last_kernel(b1_ref, v_ref, z_ref):
    rows = z_ref.shape[0]
    b1 = b1_ref[pl.ds(pl.multiple_of(lax.axis_index("mx") * rows, rows), rows), :]
    v = jnp.swapaxes(v_ref[...].astype(F32), 0, 1).astype(BF16)
    outs = [jnp.dot(b1, v[q], preferred_element_type=F32) for q in range(v.shape[0])]
    z_ref[...] = jnp.swapaxes(jnp.stack(outs, 0), 0, 1)


def solution(mesh):
    vol_spec = P("mx", "my", "mz", "rhs")
    core_spec = P("mx", "my", "mz")
    full_spec = P()
    n_m, n_x, n_y = mesh.shape["mx"], mesh.shape["my"], mesh.shape["mz"]
    groups = 1

    def local_operator(x_blk, fac_a1, fac_a2, fac_a3, diag_blk, fac_b1, fac_b2, fac_b3):
        na, nb, nc = x_blk.shape[:3]
        m1, m2, m3 = fac_a1.shape[0], fac_a2.shape[0], fac_a3.shape[0]
        x3 = x_blk.reshape(na, nb, nc)
        d_t = jnp.transpose(diag_blk, (1, 2, 0))
        n_chunk = nb // n_m // CHUNK
        ib, jb = m1 // (n_m * n_x), m2 // n_y
        im = m1 // n_m
        dj, dk, _ = d_t.shape
        n_row = n_m * n_x - 1
        vm = pltpu.VMEM
        dma = pltpu.SemaphoreType.DMA
        scratch = [
            vm((n_chunk, n_m, na, CHUNK, nc), BF16),
            vm((CHUNK, n_m * na, nc), BF16),
            vm((CHUNK, m1, nc), F32),
            vm((n_chunk, m1, CHUNK, nc), BF16),
            vm((n_m * n_x, n_chunk, ib, CHUNK, nc), BF16),
            vm((ib, m2, nc), BF16),
            vm((n_y, ib, jb, nc), BF16),
            vm((dj, im, dk), F32),
            vm((n_x, dj, ib, dk), F32),
            vm((n_y, dj, ib, dk), F32),
            vm((ib, dj, dk * n_y), F32),
            vm((n_x, ib, m2, m3), BF16),
            vm((im, nb, nc), BF16),
            dma((n_chunk,)),
            dma((2, n_chunk)),
            dma((2, n_x - 1)),
            dma((2, n_y - 1)),
            dma((2, n_chunk, groups, n_row)),
            dma((2, groups, n_y - 1)),
            dma((2, 2, max(n_x, n_y) - 1)),
            dma((2, 2, max(n_x, n_y) - 1)),
            dma((2, n_x)),
            dma((n_x,)),
        ]
        hbm = pl.BlockSpec(memory_space=pl.ANY)
        v_spec = pl.BlockSpec(memory_space=pltpu.VMEM)
        v2 = pl.pallas_call(
            functools.partial(core_kernel, (n_m, n_x, n_y, groups)),
            out_shape=jax.ShapeDtypeStruct((m1, nb, nc), BF16),
            in_specs=[hbm] + [v_spec] * 6,
            out_specs=hbm,
            scratch_shapes=scratch,
            compiler_params=pltpu.CompilerParams(
                collective_id=0, has_side_effects=True, vmem_limit_bytes=60 * 1024 * 1024),
            name="compress_expand",
        )(x3, fac_a1, fac_a2, fac_a3, d_t, fac_b2, fac_b3)
        jblk = 16
        z = pl.pallas_call(
            last_kernel,
            out_shape=jax.ShapeDtypeStruct((na, nb, nc), F32),
            grid=(nb // jblk,),
            in_specs=[pl.BlockSpec(fac_b1.shape, lambda j: (0, 0)),
                      pl.BlockSpec((m1, jblk, nc), lambda j: (0, j, 0))],
            out_specs=pl.BlockSpec((na, jblk, nc), lambda j: (0, j, 0)),
            name="last_mode",
        )(fac_b1, v2)
        return z.reshape(na, nb, nc, 1)

    return jax.shard_map(
        local_operator, mesh=mesh,
        in_specs=(vol_spec, full_spec, full_spec, full_spec, core_spec, full_spec, full_spec, full_spec),
        out_specs=vol_spec, check_vma=False)
```

```python
import functools

import jax
import jax.numpy as jnp
from jax import lax
from jax.experimental import pallas as pl
from jax.experimental.pallas import tpu as pltpu
from jax.sharding import PartitionSpec as P

MESH = pl.DeviceIdType.MESH
F32 = jnp.float32
BF16 = jnp.bfloat16
CHUNK = 16
NT = (((1,), (1,)), ((), ()))


def core_kernel(sizes, x_hbm, a1_hbm, a2_hbm, a3_hbm, d_hbm, b2_hbm, b3_hbm, v2_hbm,
                a1_ref, a2_ref, a3_ref, d_ref, b2_ref, b3_ref,
                xb, xs, uf, u1, u1r, u2, u2r, dsend, dmid, drecv, dfull, wg, v2s,
                sem_f, sem_lx, sem_x, sem_d1, sem_d2, sem_u1, sem_u2, sem_w0, sem_w1, sem_v, sem_lv):
    n_m, n_x, n_y, groups = sizes
    m, xx, yy = lax.axis_index("mx"), lax.axis_index("my"), lax.axis_index("mz")
    rows_a = x_hbm.shape[0]
    half = x_hbm.shape[1] // n_m
    n_chunk = half // CHUNK
    m1 = a1_ref.shape[0]
    ib = m1 // (n_m * n_x)
    ig = ib // groups
    jb = u2r.shape[2]
    im = ib * n_x

    def shift(dm=0, dx=0, dy=0):
        return {"mx": lax.rem(m + dm, n_m), "my": lax.rem(xx + dx, n_x), "mz": lax.rem(yy + dy, n_y)}

    def remote(src, dst, sems, idx, dev):
        cp = pltpu.make_async_remote_copy(
            src_ref=src, dst_ref=dst, send_sem=sems.at[(0,) + idx], recv_sem=sems.at[(1,) + idx],
            device_id=dev, device_id_type=MESH)
        cp.start()
        sent.append(cp)
        return cp

    def local(src, dst, sem):
        cp = pltpu.make_async_copy(src, dst, sem)
        cp.start()
        return cp

    sent = []
    row = [(dm, dx) for dx in range(n_x) for dm in range(n_m) if (dm, dx) != (0, 0)]

    barrier = pltpu.get_barrier_semaphore()
    for dm, dx in row:
        pl.semaphore_signal(barrier, inc=1, device_id=shift(dm, dx), device_id_type=MESH)
    for dy in range(1, n_y):
        pl.semaphore_signal(barrier, inc=1, device_id=shift(dy=dy), device_id_type=MESH)
    fac = [local(src, dst, sem_f.at[n]) for n, (src, dst) in enumerate(
        [(d_hbm, d_ref), (a1_hbm, a1_ref), (a2_hbm, a2_ref), (a3_hbm, a3_ref), (b2_hbm, b2_ref), (b3_hbm, b3_ref)])]
    loads = [local(x_hbm.at[:, pl.ds(m * half + q * CHUNK, CHUNK), :], xb.at[q, m], sem_lx.at[q])
             for q in range(n_chunk)]

    def swap_in(q, s):
        @pl.loop(0, rows_a // 128)
        def _(c):
            v = xb[q, s, pl.ds(pl.multiple_of(c * 128, 128), 128)].astype(F32)
            at = pl.multiple_of(s * rows_a + c * 128, 128)
            xs[:, pl.ds(at, 128), :] = jnp.swapaxes(v, 0, 1).astype(BF16)

    dk = d_ref.shape[1]
    pack = dsend.shape[2] // dk
    nq = dsend.shape[0]
    with jax.named_scope("d_prep"):
        fac[0].wait()
        parts = [jnp.swapaxes(d_ref[pl.ds(p * nq, nq)], 1, 2) for p in range(pack)]
        dsend[...] = jnp.concatenate(parts, axis=2)
        dmid[xx] = dsend[:, pl.ds(pl.multiple_of(xx * ib, ib), ib), :]
    with jax.named_scope("swap_own"):
        loads[0].wait()
        swap_in(0, m)
    with jax.named_scope("barrier"):
        pl.semaphore_wait(barrier, len(row) + n_y - 1)

    x_cp = [remote(x_hbm.at[:, pl.ds((1 - m) * half + q * CHUNK, CHUNK), :], xb.at[q, m], sem_x, (q,), shift(dm=1))
            for q in range(n_chunk)]
    d1_cp = []
    for dx in range(1, n_x):
        to = lax.rem(xx + dx, n_x)
        d1_cp.append(remote(dsend.at[:, pl.ds(to * ib, ib), :], dmid.at[xx], sem_d1, (dx - 1,), shift(dx=dx)))
    d2_cp = []

    me = xx * n_m + m
    u1_cp = [[] for _ in range(groups)]

    def send_u1(q, g):
        for r, (dm, dx) in enumerate(row):
            base = lax.rem(m + dm, n_m) * im + lax.rem(xx + dx, n_x) * ib + g * ig
            u1_cp[g].append(remote(u1.at[q, pl.ds(base, ig)], u1r.at[me, q, pl.ds(g * ig, ig)],
                                   sem_u1, (q, g, r), shift(dm, dx)))

    def mode1(q):
        if q:
            with jax.named_scope("swap_own"):
                loads[q].wait()
                swap_in(q, m)
        with jax.named_scope("x_wait"):
            x_cp[q].wait_recv()
        with jax.named_scope("swap_in"):
            swap_in(q, 1 - m)
        if q == 0:
            fac[1].wait()
        with jax.named_scope("dot1"):
            @pl.loop(0, CHUNK // 2, unroll=4)
            def _(b):
                rhs = jnp.concatenate([xs[2 * b], xs[2 * b + 1]], axis=1)
                out = jnp.dot(a1_ref[...], rhs, preferred_element_type=F32)
                lanes = out.shape[1] // 2
                uf[2 * b] = out[:, :lanes]
                uf[2 * b + 1] = out[:, lanes:]
        with jax.named_scope("swap_out"):
            step = m1 // 4

            @pl.loop(0, 4)
            def _(c):
                v = uf[:, pl.ds(pl.multiple_of(c * step, step), step), :]
                u1[q, pl.ds(c * step, step)] = jnp.swapaxes(v, 0, 1).astype(BF16)
        u1r[me, q] = u1[q, pl.ds(m * im + xx * ib, ib)]

    u2_cp = [[] for _ in range(groups)]

    def mode2(g):
        with jax.named_scope("u1_wait"):
            for cp in u1_cp[g]:
                cp.wait_recv()
        with jax.named_scope("dot2"):
            @pl.loop(0, ig // 2, unroll=2)
            def _(t):
                i = g * ig + 2 * t
                parts = [u1r[:, :, i + h].reshape(-1, u1r.shape[-1]) for h in range(2)]
                out = jnp.dot(a2_ref[...], jnp.concatenate(parts, axis=1), preferred_element_type=F32)
                lanes = out.shape[1] // 2
                u2[i] = out[:, :lanes].astype(BF16)
                u2[i + 1] = out[:, lanes:].astype(BF16)

        isl = pl.ds(g * ig, ig)
        for dy in range(1, n_y):
            to = lax.rem(yy + dy, n_y)
            u2_cp[g].append(remote(u2.at[isl, pl.ds(to * jb, jb), :], u2r.at[yy, isl],
                                   sem_u2, (g, dy - 1), shift(dy=dy)))
        u2r[yy, isl] = u2[isl, pl.ds(pl.multiple_of(yy * jb, jb), jb), :]

    jy = pl.ds(pl.multiple_of(yy * jb, jb), jb)
    hg = ig // 2
    w0 = [([], []) for _ in range(groups)]
    w1 = [([], []) for _ in range(groups)]

    def mode3(g):
        with jax.named_scope("u2_wait"):
            for cp in u2_cp[g]:
                cp.wait_recv()
        with jax.named_scope("dot3"):
            isl = pl.ds(g * ig, ig)
            parts = [u2r[s, isl].reshape(ig * jb, -1) for s in range(n_y)]
            out = lax.dot_general(jnp.concatenate(parts, axis=1), a3_ref[...], NT, preferred_element_type=F32)
            u3 = out.astype(BF16).astype(F32).reshape(ig, jb, -1)
            wg[xx, isl, jy, :] = (dfull[isl] * u3).astype(BF16)
        for dy in range(1, n_y):
            ref = wg.at[xx, pl.ds(g * ig, hg), jy, :]
            w0[g][0].append(remote(ref, ref, sem_w0, (g, 0, dy - 1), shift(dy=dy)))
        for dx in range(1, n_x):
            ref = wg.at[xx, pl.ds(g * ig + hg, hg), jy, :]
            w1[g][0].append(remote(ref, ref, sem_w1, (g, 0, dx - 1), shift(dx=dx)))

    def gather2(g):
        with jax.named_scope("w_wait1"):
            for cp in w0[g][0]:
                cp.wait_recv()
        for dx in range(1, n_x):
            ref = wg.at[xx, pl.ds(g * ig, hg)]
            w0[g][1].append(remote(ref, ref, sem_w0, (g, 1, dx - 1), shift(dx=dx)))
        with jax.named_scope("w_wait2"):
            for cp in w1[g][0]:
                cp.wait_recv()
        for dy in range(1, n_y):
            ref = wg.at[:, pl.ds(g * ig + hg, hg), jy, :]
            w1[g][1].append(remote(ref, ref, sem_w1, (g, 1, dy - 1), shift(dy=dy)))

    v_cp, lv_cp = [], []

    def expand(g):
        with jax.named_scope("w_wait3"):
            for cp in w0[g][1] + w1[g][1]:
                cp.wait_recv()
        with jax.named_scope("expand"):
            b3 = b3_ref[pl.ds(pl.multiple_of(yy * b3_ref.shape[1], 128), v2s.shape[3]), :]
            b2 = b2_ref[pl.ds(pl.multiple_of(xx * b2_ref.shape[1], 128), v2s.shape[2]), :]
            pairs = ig // 2

            @pl.loop(0, n_x * pairs, unroll=4)
            def _(t):
                s = lax.div(t, pairs)
                i = g * ig + 2 * lax.rem(t, pairs)
                w = wg[s, pl.ds(i, 2)].reshape(2 * wg.shape[2], -1)
                v3 = lax.dot_general(w, b3, NT, preferred_element_type=F32).astype(BF16)
                rows = v3.shape[0] // 2
                rhs = jnp.concatenate([v3[:rows], v3[rows:]], axis=1)
                out = jnp.dot(b2, rhs, preferred_element_type=F32).astype(BF16)
                lanes = out.shape[1] // 2
                v2s[s, i] = out[:, :lanes]
                v2s[s, i + 1] = out[:, lanes:]

        src = v2s.at[:, pl.ds(g * ig, ig)]
        dst = v2_hbm.at[m, :, pl.ds(g * ig, ig)]
        v_cp.append(remote(src, dst, sem_v, (g,), shift(dm=1)))
        lv_cp.append(local(src, dst, sem_lv.at[g]))

    def send_all(g):
        for q in range(n_chunk):
            send_u1(q, g)

    early = min(2, groups)
    for q in range(n_chunk):
        mode1(q)
        for g in range(early):
            send_u1(q, g)
        if q == 1:
            for cp in d1_cp:
                cp.wait_recv()
            for dy in range(1, n_y):
                to = lax.rem(yy + dy, n_y)
                d2_cp.append(remote(dmid.at[to], drecv.at[yy], sem_d2, (dy - 1,), shift(dy=dy)))
            drecv[yy] = dmid[yy]
    send_all(2)
    with jax.named_scope("d_full"):
        for cp in d2_cp:
            cp.wait_recv()
        parts = [jnp.concatenate([drecv[s, :, :, p * dk:(p + 1) * dk] for s in range(n_y)], axis=2)
                 for p in range(pack)]
        dfull[...] = jnp.swapaxes(jnp.concatenate(parts, axis=0), 0, 1)
    for cp in fac[2:]:
        cp.wait()
    mode2(0)
    mode2(1)
    mode3(0)
    mode3(1)
    send_all(3)
    mode2(2)
    gather2(0)
    gather2(1)
    mode3(2)
    mode2(3)
    gather2(2)
    expand(0)
    mode3(3)
    expand(1)
    gather2(3)
    expand(2)
    expand(3)
    with jax.named_scope("v_wait"):
        for cp in lv_cp:
            cp.wait()
        for cp in v_cp:
            cp.wait_recv()
    for cp in sent:
        cp.wait_send()


def last_kernel(b1_ref, v_ref, z_ref):
    rows = z_ref.shape[0]
    b1 = b1_ref[pl.ds(pl.multiple_of(lax.axis_index("mx") * rows, rows), rows), :]
    v = jnp.swapaxes(v_ref[...].astype(F32), 0, 1).astype(BF16)
    outs = [jnp.dot(b1, v[q], preferred_element_type=F32) for q in range(v.shape[0])]
    z_ref[...] = jnp.swapaxes(jnp.stack(outs, 0), 0, 1)


def solution(mesh):
    vol_spec = P("mx", "my", "mz", "rhs")
    core_spec = P("mx", "my", "mz")
    full_spec = P()
    n_m, n_x, n_y = mesh.shape["mx"], mesh.shape["my"], mesh.shape["mz"]
    groups = 4

    def local_operator(x_blk, fac_a1, fac_a2, fac_a3, diag_blk, fac_b1, fac_b2, fac_b3):
        na, nb, nc = x_blk.shape[:3]
        m1, m2, m3 = fac_a1.shape[0], fac_a2.shape[0], fac_a3.shape[0]
        x3 = x_blk.reshape(na, nb, nc)
        d_t = jnp.transpose(diag_blk, (1, 2, 0))
        n_chunk = nb // n_m // CHUNK
        ib, jb = m1 // (n_m * n_x), m2 // n_y
        im = m1 // n_m
        dj, dk, _ = d_t.shape
        n_row = n_m * n_x - 1
        vm = pltpu.VMEM
        dma = pltpu.SemaphoreType.DMA
        pack = nc // dk
        scratch = [
            vm(fac_a1.shape, BF16),
            vm(fac_a2.shape, BF16),
            vm(fac_a3.shape, BF16),
            vm(d_t.shape, F32),
            vm(fac_b2.shape, BF16),
            vm(fac_b3.shape, BF16),
            vm((n_chunk, n_m, na, CHUNK, nc), BF16),
            vm((CHUNK, n_m * na, nc), BF16),
            vm((CHUNK, m1, nc), F32),
            vm((n_chunk, m1, CHUNK, nc), BF16),
            vm((n_m * n_x, n_chunk, ib, CHUNK, nc), BF16),
            vm((ib, m2, nc), BF16),
            vm((n_y, ib, jb, nc), BF16),
            vm((dj // pack, im, dk * pack), F32),
            vm((n_x, dj // pack, ib, dk * pack), F32),
            vm((n_y, dj // pack, ib, dk * pack), F32),
            vm((ib, dj, dk * n_y), F32),
            vm((n_x, ib, m2, m3), BF16),
            vm((n_x, ib, nb, nc), BF16),
            dma((6,)),
            dma((n_chunk,)),
            dma((2, n_chunk)),
            dma((2, n_x - 1)),
            dma((2, n_y - 1)),
            dma((2, n_chunk, groups, n_row)),
            dma((2, groups, n_y - 1)),
            dma((2, groups, 2, max(n_x, n_y) - 1)),
            dma((2, groups, 2, max(n_x, n_y) - 1)),
            dma((2, groups)),
            dma((groups,)),
        ]
        hbm = pl.BlockSpec(memory_space=pl.ANY)
        v2 = pl.pallas_call(
            functools.partial(core_kernel, (n_m, n_x, n_y, groups)),
            out_shape=jax.ShapeDtypeStruct((n_m, n_x, ib, nb, nc), BF16),
            in_specs=[hbm] * 7,
            out_specs=hbm,
            scratch_shapes=scratch,
            compiler_params=pltpu.CompilerParams(
                collective_id=0, has_side_effects=True, vmem_limit_bytes=60 * 1024 * 1024),
            name="compress_expand",
        )(x3, fac_a1, fac_a2, fac_a3, d_t, fac_b2, fac_b3)
        jblk = 16
        z = pl.pallas_call(
            last_kernel,
            out_shape=jax.ShapeDtypeStruct((na, nb, nc), F32),
            grid=(nb // jblk,),
            in_specs=[pl.BlockSpec(fac_b1.shape, lambda j: (0, 0)),
                      pl.BlockSpec((m1, jblk, nc), lambda j: (0, j, 0))],
            out_specs=pl.BlockSpec((na, jblk, nc), lambda j: (0, j, 0)),
            name="last_mode",
        )(fac_b1, v2.reshape(m1, nb, nc))
        return z.reshape(na, nb, nc, 1)

    return jax.shard_map(
        local_operator, mesh=mesh,
        in_specs=(vol_spec, full_spec, full_spec, full_spec, core_spec, full_spec, full_spec, full_spec),
        out_specs=vol_spec, check_vma=False)
```

```python
import functools

import jax
import jax.numpy as jnp
from jax import lax
from jax.experimental import pallas as pl
from jax.experimental.pallas import tpu as pltpu
from jax.sharding import PartitionSpec as P

MESH = pl.DeviceIdType.MESH
F32 = jnp.float32
BF16 = jnp.bfloat16
CHUNK = 16
NT = (((1,), (1,)), ((), ()))
ORDER = (
    "C0", "S02", "S01", "S00", "C1", "S12", "S10", "C2", "T", "S20", "C3", "S30", "S11", "S31", "S21", "S32",
    "S22", "M0", "S33", "M1", "D", "W0", "S13", "M2", "S03", "S23", "W1", "P00", "P01", "W2", "M3", "P11",
    "P10", "W3", "P21", "P20", "P30", "P31", "E0", "E1", "E2", "E3",
)


def core_kernel(sizes, x_hbm, a1_hbm, a2_hbm, a3_hbm, d_hbm, b2_hbm, b3_hbm, v2_hbm,
                a1_ref, a2_ref, a3_ref, d_ref, b2_ref, b3_ref,
                xb, xs, uf, u1, u1r, u2, u2r, dsend, dmid, drecv, dfull, wg, vf, v2s,
                sem_f, sem_lx, sem_x, sem_d1, sem_d2, sem_u1, sem_u2, sem_w0, sem_w1, sem_v, sem_lv):
    n_m, n_x, n_y, groups = sizes
    m, xx, yy = lax.axis_index("mx"), lax.axis_index("my"), lax.axis_index("mz")
    rows_a = x_hbm.shape[0]
    half = x_hbm.shape[1] // n_m
    n_chunk = half // CHUNK
    m1 = a1_ref.shape[0]
    ib = m1 // (n_m * n_x)
    ig = ib // groups
    jb = u2r.shape[2]
    im = ib * n_x

    def shift(dm=0, dx=0, dy=0):
        return {"mx": lax.rem(m + dm, n_m), "my": lax.rem(xx + dx, n_x), "mz": lax.rem(yy + dy, n_y)}

    def remote(src, dst, sems, idx, dev):
        cp = pltpu.make_async_remote_copy(
            src_ref=src, dst_ref=dst, send_sem=sems.at[(0,) + idx], recv_sem=sems.at[(1,) + idx],
            device_id=dev, device_id_type=MESH)
        cp.start()
        sent.append(cp)
        return cp

    def local(src, dst, sem):
        cp = pltpu.make_async_copy(src, dst, sem)
        cp.start()
        return cp

    sent = []
    far_x = sorted(range(1, n_x), key=lambda d: (min(d, n_x - d), d))
    far_y = sorted(range(1, n_y), key=lambda d: (min(d, n_y - d), d))
    row = [(dm, dx) for dm in range(n_m) for dx in far_x] + [(dm, 0) for dm in range(1, n_m)]

    barrier = pltpu.get_barrier_semaphore()
    for dm, dx in row:
        pl.semaphore_signal(barrier, inc=1, device_id=shift(dm, dx), device_id_type=MESH)
    for dy in range(1, n_y):
        pl.semaphore_signal(barrier, inc=1, device_id=shift(dy=dy), device_id_type=MESH)
    fac = [local(src, dst, sem_f.at[n]) for n, (src, dst) in enumerate(
        [(d_hbm, d_ref), (a1_hbm, a1_ref), (a2_hbm, a2_ref), (a3_hbm, a3_ref), (b2_hbm, b2_ref), (b3_hbm, b3_ref)])]
    loads = [local(x_hbm.at[:, pl.ds(m * half + q * CHUNK, CHUNK), :], xb.at[q, m], sem_lx.at[q])
             for q in range(n_chunk)]

    def swap_in(q, s):
        @pl.loop(0, rows_a // 128)
        def _(c):
            v = xb[q, s, pl.ds(pl.multiple_of(c * 128, 128), 128)].astype(F32)
            at = pl.multiple_of(s * rows_a + c * 128, 128)
            xs[:, pl.ds(at, 128), :] = jnp.swapaxes(v, 0, 1).astype(BF16)

    dk = d_ref.shape[1]
    pack = dsend.shape[4] // dk
    nq = dsend.shape[3]
    with jax.named_scope("d_prep"):
        fac[0].wait()
        parts = [jnp.swapaxes(d_ref[pl.ds(p * nq, nq)], 1, 2) for p in range(pack)]
        packed = jnp.swapaxes(jnp.concatenate(parts, axis=2), 0, 1)
        dsend[...] = packed.reshape(dsend.shape)
        dmid[xx] = dsend[:, xx]
    with jax.named_scope("swap_own"):
        loads[0].wait()
        swap_in(0, m)
    with jax.named_scope("barrier"):
        pl.semaphore_wait(barrier, len(row) + n_y - 1)

    d1_cp = []
    for dx in range(1, n_x):
        to = lax.rem(xx + dx, n_x)
        d1_cp.append(remote(dsend.at[:, to], dmid.at[xx], sem_d1, (dx - 1,), shift(dx=dx)))
    x_cp = []

    def send_x(q):
        x_cp.append(remote(x_hbm.at[:, pl.ds((1 - m) * half + q * CHUNK, CHUNK), :], xb.at[q, m],
                           sem_x, (q,), shift(dm=1)))

    send_x(0)
    d2_cp = []

    me = xx * n_m + m
    u1_cp = [[] for _ in range(groups)]

    def send_u1(q, g):
        for r, (dm, dx) in enumerate(row):
            base = lax.rem(m + dm, n_m) * im + g * ig * n_x + lax.rem(xx + dx, n_x) * ig
            u1_cp[g].append(remote(u1.at[q, pl.ds(base, ig)], u1r.at[me, q, pl.ds(g * ig, ig)],
                                   sem_u1, (q, g, r), shift(dm, dx)))

    def mode1(q):
        if q:
            with jax.named_scope("swap_own"):
                loads[q].wait()
                swap_in(q, m)
        with jax.named_scope("x_wait"):
            x_cp[q].wait_recv()
        if q + 1 < n_chunk:
            send_x(q + 1)
        with jax.named_scope("swap_in"):
            swap_in(q, 1 - m)
        for cp in fac[1:] if q == 0 else []:
            cp.wait()
        with jax.named_scope("dot1"):
            @pl.loop(0, CHUNK // 2, unroll=8)
            def _(b):
                rhs = jnp.concatenate([xs[2 * b], xs[2 * b + 1]], axis=1)
                out = jnp.dot(a1_ref[...], rhs, preferred_element_type=F32)
                lanes = out.shape[1] // 2
                uf[2 * b] = out[:, :lanes]
                uf[2 * b + 1] = out[:, lanes:]
        with jax.named_scope("swap_out"):
            step = m1 // 4

            @pl.loop(0, 4)
            def _(c):
                v = uf[:, pl.ds(pl.multiple_of(c * step, step), step), :]
                u1[q, pl.ds(c * step, step)] = jnp.swapaxes(v, 0, 1).astype(BF16)
        for g in range(groups):
            u1r[me, q, pl.ds(g * ig, ig)] = u1[q, pl.ds(m * im + g * ig * n_x + xx * ig, ig)]

    u2_cp = [[] for _ in range(groups)]

    def mode2(g):
        with jax.named_scope("u1_wait"):
            for cp in u1_cp[g]:
                cp.wait_recv()
        with jax.named_scope("dot2"):
            @pl.loop(0, ig // 2, unroll=2)
            def _(t):
                i = g * ig + 2 * t
                parts = [u1r[:, :, i + h].reshape(-1, u1r.shape[-1]) for h in range(2)]
                out = jnp.dot(a2_ref[...], jnp.concatenate(parts, axis=1), preferred_element_type=F32)
                lanes = out.shape[1] // 2
                u2[i] = out[:, :lanes].astype(BF16)
                u2[i + 1] = out[:, lanes:].astype(BF16)

        isl = pl.ds(g * ig, ig)
        for dy in far_y:
            to = lax.rem(yy + dy, n_y)
            u2_cp[g].append(remote(u2.at[isl, pl.ds(to * jb, jb), :], u2r.at[yy, isl],
                                   sem_u2, (g, dy - 1), shift(dy=dy)))
        u2r[yy, isl] = u2[isl, pl.ds(pl.multiple_of(yy * jb, jb), jb), :]

    jy = pl.ds(pl.multiple_of(yy * jb, jb), jb)
    hg = ig // 2
    w0 = [([], []) for _ in range(groups)]
    w1 = [([], []) for _ in range(groups)]

    def mode3(g):
        with jax.named_scope("u2_wait"):
            for cp in u2_cp[g]:
                cp.wait_recv()
        with jax.named_scope("dot3"):
            isl = pl.ds(g * ig, ig)
            parts = [u2r[s, isl].reshape(ig * jb, -1) for s in range(n_y)]
            out = lax.dot_general(jnp.concatenate(parts, axis=1), a3_ref[...], NT, preferred_element_type=F32)
            u3 = out.astype(BF16).astype(F32).reshape(ig, jb, -1)
            wg[xx, isl, jy, :] = (dfull[isl] * u3).astype(BF16)
        for dy in far_y:
            ref = wg.at[xx, pl.ds(g * ig, hg), jy, :]
            w0[g][0].append(remote(ref, ref, sem_w0, (g, 0, dy - 1), shift(dy=dy)))
        for dx in far_x:
            ref = wg.at[xx, pl.ds(g * ig + hg, hg), jy, :]
            w1[g][0].append(remote(ref, ref, sem_w1, (g, 0, dx - 1), shift(dx=dx)))

    def gather2(g, k):
        with jax.named_scope(f"p_wait{k}_{g}"):
            for cp in (w0, w1)[k][g][0]:
                cp.wait_recv()
        if k == 0:
            ref = wg.at[xx, pl.ds(g * ig, hg)]
            for dx in far_x:
                w0[g][1].append(remote(ref, ref, sem_w0, (g, 1, dx - 1), shift(dx=dx)))
        else:
            ref = wg.at[:, pl.ds(g * ig + hg, hg), jy, :]
            for dy in far_y:
                w1[g][1].append(remote(ref, ref, sem_w1, (g, 1, dy - 1), shift(dy=dy)))

    v_cp, lv_cp = [], []

    def expand(g):
        with jax.named_scope("w_wait3"):
            for cp in w0[g][1] + w1[g][1]:
                cp.wait_recv()
        with jax.named_scope("expand"):
            b3 = b3_ref[pl.ds(pl.multiple_of(yy * b3_ref.shape[1], 128), v2s.shape[2]), :]
            b2 = b2_ref[pl.ds(pl.multiple_of(xx * b2_ref.shape[1], 128), v2s.shape[0]), :]
            pairs = ig // 2

            @pl.loop(0, n_x * pairs, unroll=8)
            def _(t):
                s = lax.div(t, pairs)
                i = g * ig + 2 * lax.rem(t, pairs)
                w = wg[s, pl.ds(i, 2)].reshape(2 * wg.shape[2], -1)
                v3 = lax.dot_general(w, b3, NT, preferred_element_type=F32).astype(BF16)
                rows = v3.shape[0] // 2
                rhs = jnp.concatenate([v3[:rows], v3[rows:]], axis=1)
                out = jnp.dot(b2, rhs, preferred_element_type=F32)
                lanes = out.shape[1] // 2
                vf[2 * t] = out[:, :lanes]
                vf[2 * t + 1] = out[:, lanes:]

        base = g * ig * n_x
        step = vf.shape[1] // 4
        with jax.named_scope("swap_v"):
            @pl.loop(0, 4)
            def _(c):
                at = pl.multiple_of(c * step, step)
                v2s[pl.ds(at, step), pl.ds(base, ig * n_x), :] = jnp.swapaxes(
                    vf[:, pl.ds(at, step), :], 0, 1).astype(BF16)
        src = v2s.at[:, pl.ds(base, ig * n_x), :]
        dst = v2_hbm.at[:, pl.ds(m * im + base, ig * n_x), :]
        v_cp.append(remote(src, dst, sem_v, (g,), shift(dm=1)))
        lv_cp.append(local(src, dst, sem_lv.at[g]))

    def diag_turn():
        with jax.named_scope("d1_wait"):
            for cp in d1_cp:
                cp.wait_recv()
        for dy in range(1, n_y):
            to = lax.rem(yy + dy, n_y)
            d2_cp.append(remote(dmid.at[to], drecv.at[yy], sem_d2, (dy - 1,), shift(dy=dy)))
        drecv[yy] = dmid[yy]

    def diag_full():
        with jax.named_scope("d_full"):
            for cp in d2_cp:
                cp.wait_recv()
            lanes = [drecv[s].reshape(ib, nq, -1) for s in range(n_y)]
            parts = [jnp.concatenate([v[:, :, p * dk:(p + 1) * dk] for v in lanes], axis=2) for p in range(pack)]
            dfull[...] = jnp.concatenate(parts, axis=1)

    steps = {"C": mode1, "S": send_u1, "T": diag_turn, "D": diag_full, "M": mode2, "W": mode3,
             "P": gather2, "E": expand}
    for word in ORDER:
        steps[word[0]](*[int(c) for c in word[1:]])
    with jax.named_scope("v_wait"):
        for cp in lv_cp:
            cp.wait()
        for cp in v_cp:
            cp.wait_recv()
    for cp in sent:
        cp.wait_send()


def last_kernel(b1_ref, v_ref, z_hbm, buf, sem):
    rows = buf.shape[2]
    s, n = pl.program_id(0), pl.num_programs(0)
    slot = lax.rem(s, 2)
    width = v_ref.shape[0]

    def drain(k):
        pltpu.make_async_copy(buf.at[k], buf.at[k], sem.at[k]).wait()

    @pl.when(s >= 2)
    def _():
        drain(slot)

    b1 = b1_ref[pl.ds(pl.multiple_of(lax.axis_index("mx") * rows, rows), rows), :]
    for q in range(0, width, 2):
        rhs = jnp.concatenate([v_ref[q], v_ref[q + 1]], axis=1)
        out = jnp.dot(b1, rhs, preferred_element_type=F32)
        lanes = out.shape[1] // 2
        for h in range(2):
            buf[slot, q + h] = out[:, h * lanes:(h + 1) * lanes]
            pltpu.make_async_copy(buf.at[slot, q + h], z_hbm.at[:, s * width + q + h, 0, :], sem.at[slot]).start()

    @pl.when(s == n - 1)
    def _():
        drain(0)
        drain(1)


def solution(mesh):
    vol_spec = P("mx", "my", "mz", "rhs")
    core_spec = P("mx", "my", "mz")
    full_spec = P()
    n_m, n_x, n_y = mesh.shape["mx"], mesh.shape["my"], mesh.shape["mz"]
    groups = 4

    def local_operator(x_blk, fac_a1, fac_a2, fac_a3, diag_blk, fac_b1, fac_b2, fac_b3):
        na, nb, nc = x_blk.shape[:3]
        m1, m2, m3 = fac_a1.shape[0], fac_a2.shape[0], fac_a3.shape[0]
        x3 = x_blk.reshape(na, nb, nc)
        d_t = jnp.transpose(diag_blk, (1, 2, 0))
        n_chunk = nb // n_m // CHUNK
        ib, jb = m1 // (n_m * n_x), m2 // n_y
        im = m1 // n_m
        dj, dk, _ = d_t.shape
        n_row = n_m * n_x - 1
        vm = pltpu.VMEM
        dma = pltpu.SemaphoreType.DMA
        pack = nc // dk
        scratch = [
            vm(fac_a1.shape, BF16),
            vm(fac_a2.shape, BF16),
            vm(fac_a3.shape, BF16),
            vm(d_t.shape, F32),
            vm(fac_b2.shape, BF16),
            vm(fac_b3.shape, BF16),
            vm((n_chunk, n_m, na, CHUNK, nc), BF16),
            vm((CHUNK, n_m * na, nc), BF16),
            vm((CHUNK, m1, nc), F32),
            vm((n_chunk, m1, CHUNK, nc), BF16),
            vm((n_m * n_x, n_chunk, ib, CHUNK, nc), BF16),
            vm((ib, m2, nc), BF16),
            vm((n_y, ib, jb, nc), BF16),
            vm((groups, n_x, ib // groups, dj // pack, dk * pack), F32),
            vm((n_x, groups, ib // groups, dj // pack, dk * pack), F32),
            vm((n_y, groups, ib // groups, dj // pack, dk * pack), F32),
            vm((ib, dj, dk * n_y), F32),
            vm((n_x, ib, m2, m3), BF16),
            vm((im // groups, nb, nc), F32),
            vm((nb, im, nc), BF16),
            dma((6,)),
            dma((n_chunk,)),
            dma((2, n_chunk)),
            dma((2, n_x - 1)),
            dma((2, n_y - 1)),
            dma((2, n_chunk, groups, n_row)),
            dma((2, groups, n_y - 1)),
            dma((2, groups, 2, max(n_x, n_y) - 1)),
            dma((2, groups, 2, max(n_x, n_y) - 1)),
            dma((2, groups)),
            dma((groups,)),
        ]
        hbm = pl.BlockSpec(memory_space=pl.ANY)
        v2 = pl.pallas_call(
            functools.partial(core_kernel, (n_m, n_x, n_y, groups)),
            out_shape=jax.ShapeDtypeStruct((nb, m1, nc), BF16),
            in_specs=[hbm] * 7,
            out_specs=hbm,
            scratch_shapes=scratch,
            compiler_params=pltpu.CompilerParams(
                collective_id=0, has_side_effects=True, vmem_limit_bytes=60 * 1024 * 1024),
            name="compress_expand",
        )(x3, fac_a1, fac_a2, fac_a3, d_t, fac_b2, fac_b3)
        jblk = 32
        z = pl.pallas_call(
            last_kernel,
            out_shape=jax.ShapeDtypeStruct((na, nb, 1, nc), F32),
            grid=(nb // jblk,),
            in_specs=[pl.BlockSpec(fac_b1.shape, lambda j: (0, 0)),
                      pl.BlockSpec((jblk, m1, nc), lambda j: (j, 0, 0))],
            out_specs=hbm,
            scratch_shapes=[vm((2, jblk, na, nc), F32), dma((2,))],
            compiler_params=pltpu.CompilerParams(vmem_limit_bytes=48 * 1024 * 1024),
            name="last_mode",
        )(fac_b1, v2)
        return z.reshape(na, nb, nc, 1)

    return jax.shard_map(
        local_operator, mesh=mesh,
        in_specs=(vol_spec, full_spec, full_spec, full_spec, core_spec, full_spec, full_spec, full_spec),
        out_specs=vol_spec, check_vma=False)
```

```python
import functools

import jax
import jax.numpy as jnp
from jax import lax
from jax.experimental import pallas as pl
from jax.experimental.pallas import tpu as pltpu
from jax.sharding import PartitionSpec as P

MESH = pl.DeviceIdType.MESH
F32 = jnp.float32
BF16 = jnp.bfloat16
CHUNK = 16
NT = (((1,), (1,)), ((), ()))
ORDER = (
    "C0", "S02", "S01", "S00", "C1", "S12", "S10", "C2", "T", "S20", "C3", "S30", "S11", "S31", "S21", "S32",
    "S22", "M0", "S33", "M1", "D", "W0", "S13", "M2", "S03", "S23", "W1", "P00", "P01", "W2", "M3", "P11",
    "P10", "W3", "P21", "P20", "P30", "P31", "E0", "E1", "E2", "E3",
)


def core_kernel(sizes, x_hbm, a1_hbm, a2_hbm, a3_hbm, d_hbm, b2_hbm, b3_hbm, v2_ref,
                a1_ref, a2_ref, a3_ref, d_ref, b2_ref, b3_ref,
                xb, xs, uf, u1, u1r, u2, u2r, dsend, dmid, drecv, dfull, wg, vf,
                sem_f, sem_lx, sem_x, sem_d1, sem_d2, sem_u1, sem_u2, sem_w0, sem_w1, sem_v):
    n_m, n_x, n_y, groups = sizes
    m, xx, yy = lax.axis_index("mx"), lax.axis_index("my"), lax.axis_index("mz")
    rows_a = x_hbm.shape[0]
    half = x_hbm.shape[1] // n_m
    n_chunk = half // CHUNK
    m1 = a1_ref.shape[0]
    ib = m1 // (n_m * n_x)
    ig = ib // groups
    jb = u2r.shape[2]
    im = ib * n_x

    def shift(dm=0, dx=0, dy=0):
        return {"mx": lax.rem(m + dm, n_m), "my": lax.rem(xx + dx, n_x), "mz": lax.rem(yy + dy, n_y)}

    def remote(src, dst, sems, idx, dev):
        cp = pltpu.make_async_remote_copy(
            src_ref=src, dst_ref=dst, send_sem=sems.at[(0,) + idx], recv_sem=sems.at[(1,) + idx],
            device_id=dev, device_id_type=MESH)
        cp.start()
        sent.append(cp)
        return cp

    def local(src, dst, sem):
        cp = pltpu.make_async_copy(src, dst, sem)
        cp.start()
        return cp

    sent = []
    far_x = sorted(range(1, n_x), key=lambda d: (min(d, n_x - d), d))
    far_y = sorted(range(1, n_y), key=lambda d: (min(d, n_y - d), d))
    row = [(dm, dx) for dm in range(n_m) for dx in far_x] + [(dm, 0) for dm in range(1, n_m)]

    barrier = pltpu.get_barrier_semaphore()
    for dm, dx in row:
        pl.semaphore_signal(barrier, inc=1, device_id=shift(dm, dx), device_id_type=MESH)
    for dy in range(1, n_y):
        pl.semaphore_signal(barrier, inc=1, device_id=shift(dy=dy), device_id_type=MESH)
    fac = [local(src, dst, sem_f.at[n]) for n, (src, dst) in enumerate(
        [(d_hbm, d_ref), (a1_hbm, a1_ref), (a2_hbm, a2_ref), (a3_hbm, a3_ref), (b2_hbm, b2_ref), (b3_hbm, b3_ref)])]
    loads = [local(x_hbm.at[:, pl.ds(m * half + q * CHUNK, CHUNK), :], xb.at[q, m], sem_lx.at[q])
             for q in range(n_chunk)]

    def swap_in(q, s):
        @pl.loop(0, rows_a // 128)
        def _(c):
            v = xb[q, s, pl.ds(pl.multiple_of(c * 128, 128), 128)].astype(F32)
            at = pl.multiple_of(s * rows_a + c * 128, 128)
            xs[:, pl.ds(at, 128), :] = jnp.swapaxes(v, 0, 1).astype(BF16)

    dk = d_ref.shape[1]
    pack = dsend.shape[4] // dk
    nq = dsend.shape[3]
    with jax.named_scope("d_prep"):
        fac[0].wait()
        parts = [jnp.swapaxes(d_ref[pl.ds(p * nq, nq)], 1, 2) for p in range(pack)]
        packed = jnp.swapaxes(jnp.concatenate(parts, axis=2), 0, 1)
        dsend[...] = packed.reshape(dsend.shape)
        dmid[xx] = dsend[:, xx]
    with jax.named_scope("swap_own"):
        loads[0].wait()
        swap_in(0, m)
    with jax.named_scope("barrier"):
        pl.semaphore_wait(barrier, len(row) + n_y - 1)

    d1_cp = []
    for dx in range(1, n_x):
        to = lax.rem(xx + dx, n_x)
        d1_cp.append(remote(dsend.at[:, to], dmid.at[xx], sem_d1, (dx - 1,), shift(dx=dx)))
    x_cp = []

    def send_x(q):
        x_cp.append(remote(x_hbm.at[:, pl.ds((1 - m) * half + q * CHUNK, CHUNK), :], xb.at[q, m],
                           sem_x, (q,), shift(dm=1)))

    send_x(0)
    d2_cp = []

    me = xx * n_m + m
    u1_cp = [[] for _ in range(groups)]

    def send_u1(q, g):
        for r, (dm, dx) in enumerate(row):
            base = lax.rem(m + dm, n_m) * im + g * ig * n_x + lax.rem(xx + dx, n_x) * ig
            u1_cp[g].append(remote(u1.at[q, pl.ds(base, ig)], u1r.at[me, q, pl.ds(g * ig, ig)],
                                   sem_u1, (q, g, r), shift(dm, dx)))

    def mode1(q):
        if q:
            with jax.named_scope("swap_own"):
                loads[q].wait()
                swap_in(q, m)
        with jax.named_scope("x_wait"):
            x_cp[q].wait_recv()
        if q + 1 < n_chunk:
            send_x(q + 1)
        with jax.named_scope("swap_in"):
            swap_in(q, 1 - m)
        for cp in fac[1:] if q == 0 else []:
            cp.wait()
        with jax.named_scope("dot1"):
            @pl.loop(0, CHUNK // 2, unroll=8)
            def _(b):
                rhs = jnp.concatenate([xs[2 * b], xs[2 * b + 1]], axis=1)
                out = jnp.dot(a1_ref[...], rhs, preferred_element_type=F32)
                lanes = out.shape[1] // 2
                uf[2 * b] = out[:, :lanes]
                uf[2 * b + 1] = out[:, lanes:]
        with jax.named_scope("swap_out"):
            step = m1 // 4

            @pl.loop(0, 4)
            def _(c):
                v = uf[:, pl.ds(pl.multiple_of(c * step, step), step), :]
                u1[q, pl.ds(c * step, step)] = jnp.swapaxes(v, 0, 1).astype(BF16)
        for g in range(groups):
            u1r[me, q, pl.ds(g * ig, ig)] = u1[q, pl.ds(m * im + g * ig * n_x + xx * ig, ig)]

    u2_cp = [[] for _ in range(groups)]

    def mode2(g):
        with jax.named_scope("u1_wait"):
            for cp in u1_cp[g]:
                cp.wait_recv()
        with jax.named_scope("dot2"):
            @pl.loop(0, ig // 2, unroll=2)
            def _(t):
                i = g * ig + 2 * t
                parts = [u1r[:, :, i + h].reshape(-1, u1r.shape[-1]) for h in range(2)]
                out = jnp.dot(a2_ref[...], jnp.concatenate(parts, axis=1), preferred_element_type=F32)
                lanes = out.shape[1] // 2
                u2[i] = out[:, :lanes].astype(BF16)
                u2[i + 1] = out[:, lanes:].astype(BF16)

        isl = pl.ds(g * ig, ig)
        for dy in far_y:
            to = lax.rem(yy + dy, n_y)
            u2_cp[g].append(remote(u2.at[isl, pl.ds(to * jb, jb), :], u2r.at[yy, isl],
                                   sem_u2, (g, dy - 1), shift(dy=dy)))
        u2r[yy, isl] = u2[isl, pl.ds(pl.multiple_of(yy * jb, jb), jb), :]

    jy = pl.ds(pl.multiple_of(yy * jb, jb), jb)
    hg = ig // 2
    w0 = [([], []) for _ in range(groups)]
    w1 = [([], []) for _ in range(groups)]

    def mode3(g):
        with jax.named_scope("u2_wait"):
            for cp in u2_cp[g]:
                cp.wait_recv()
        with jax.named_scope("dot3"):
            isl = pl.ds(g * ig, ig)
            parts = [u2r[s, isl].reshape(ig * jb, -1) for s in range(n_y)]
            out = lax.dot_general(jnp.concatenate(parts, axis=1), a3_ref[...], NT, preferred_element_type=F32)
            u3 = out.astype(BF16).astype(F32).reshape(ig, jb, -1)
            wg[xx, isl, jy, :] = (dfull[isl] * u3).astype(BF16)
        for dy in far_y:
            ref = wg.at[xx, pl.ds(g * ig, hg), jy, :]
            w0[g][0].append(remote(ref, ref, sem_w0, (g, 0, dy - 1), shift(dy=dy)))
        for dx in far_x:
            ref = wg.at[xx, pl.ds(g * ig + hg, hg), jy, :]
            w1[g][0].append(remote(ref, ref, sem_w1, (g, 0, dx - 1), shift(dx=dx)))

    def gather2(g, k):
        with jax.named_scope(f"p_wait{k}_{g}"):
            for cp in (w0, w1)[k][g][0]:
                cp.wait_recv()
        if k == 0:
            ref = wg.at[xx, pl.ds(g * ig, hg)]
            for dx in far_x:
                w0[g][1].append(remote(ref, ref, sem_w0, (g, 1, dx - 1), shift(dx=dx)))
        else:
            ref = wg.at[:, pl.ds(g * ig + hg, hg), jy, :]
            for dy in far_y:
                w1[g][1].append(remote(ref, ref, sem_w1, (g, 1, dy - 1), shift(dy=dy)))

    v_cp = []

    def expand(g):
        with jax.named_scope("w_wait3"):
            for cp in w0[g][1] + w1[g][1]:
                cp.wait_recv()
        with jax.named_scope("expand"):
            b3 = b3_ref[pl.ds(pl.multiple_of(yy * b3_ref.shape[1], 128), v2_ref.shape[2]), :]
            b2 = b2_ref[pl.ds(pl.multiple_of(xx * b2_ref.shape[1], 128), v2_ref.shape[0]), :]
            pairs = ig // 2

            @pl.loop(0, n_x * pairs, unroll=8)
            def _(t):
                s = lax.div(t, pairs)
                i = g * ig + 2 * lax.rem(t, pairs)
                w = wg[s, pl.ds(i, 2)].reshape(2 * wg.shape[2], -1)
                v3 = lax.dot_general(w, b3, NT, preferred_element_type=F32).astype(BF16)
                rows = v3.shape[0] // 2
                rhs = jnp.concatenate([v3[:rows], v3[rows:]], axis=1)
                out = jnp.dot(b2, rhs, preferred_element_type=F32)
                lanes = out.shape[1] // 2
                vf[2 * t] = out[:, :lanes]
                vf[2 * t + 1] = out[:, lanes:]

        mine = pl.multiple_of(m * im + g * ig * n_x, ig * n_x)
        step = vf.shape[1] // 4
        with jax.named_scope("swap_v"):
            @pl.loop(0, 4)
            def _(c):
                at = pl.multiple_of(c * step, step)
                v2_ref[pl.ds(at, step), pl.ds(mine, ig * n_x), :] = jnp.swapaxes(
                    vf[:, pl.ds(at, step), :], 0, 1).astype(BF16)
        ref = v2_ref.at[:, pl.ds(mine, ig * n_x), :]
        v_cp.append(remote(ref, ref, sem_v, (g,), shift(dm=1)))

    def diag_turn():
        with jax.named_scope("d1_wait"):
            for cp in d1_cp:
                cp.wait_recv()
        for dy in range(1, n_y):
            to = lax.rem(yy + dy, n_y)
            d2_cp.append(remote(dmid.at[to], drecv.at[yy], sem_d2, (dy - 1,), shift(dy=dy)))
        drecv[yy] = dmid[yy]

    def diag_full():
        with jax.named_scope("d_full"):
            for cp in d2_cp:
                cp.wait_recv()
            lanes = [drecv[s].reshape(ib, nq, -1) for s in range(n_y)]
            parts = [jnp.concatenate([v[:, :, p * dk:(p + 1) * dk] for v in lanes], axis=2) for p in range(pack)]
            dfull[...] = jnp.concatenate(parts, axis=1)

    steps = {"C": mode1, "S": send_u1, "T": diag_turn, "D": diag_full, "M": mode2, "W": mode3,
             "P": gather2, "E": expand}
    for word in ORDER:
        steps[word[0]](*[int(c) for c in word[1:]])
    with jax.named_scope("v_wait"):
        for cp in v_cp:
            cp.wait_recv()
    for cp in sent:
        cp.wait_send()


def last_kernel(b1_ref, v_ref, z_hbm, buf, sem):
    rows = buf.shape[2]
    s, n = pl.program_id(0), pl.num_programs(0)
    slot = lax.rem(s, 2)
    width = v_ref.shape[0]

    def drain(k):
        pltpu.make_async_copy(buf.at[k], buf.at[k], sem.at[k]).wait()

    @pl.when(s >= 2)
    def _():
        drain(slot)

    b1 = b1_ref[pl.ds(pl.multiple_of(lax.axis_index("mx") * rows, rows), rows), :]
    for q in range(0, width, 2):
        rhs = jnp.concatenate([v_ref[q], v_ref[q + 1]], axis=1)
        out = jnp.dot(b1, rhs, preferred_element_type=F32)
        lanes = out.shape[1] // 2
        for h in range(2):
            buf[slot, q + h] = out[:, h * lanes:(h + 1) * lanes]
            pltpu.make_async_copy(buf.at[slot, q + h], z_hbm.at[:, s * width + q + h, 0, :], sem.at[slot]).start()

    @pl.when(s == n - 1)
    def _():
        drain(0)
        drain(1)


def solution(mesh):
    vol_spec = P("mx", "my", "mz", "rhs")
    core_spec = P("mx", "my", "mz")
    full_spec = P()
    n_m, n_x, n_y = mesh.shape["mx"], mesh.shape["my"], mesh.shape["mz"]
    groups = 4

    def local_operator(x_blk, fac_a1, fac_a2, fac_a3, diag_blk, fac_b1, fac_b2, fac_b3):
        na, nb, nc = x_blk.shape[:3]
        m1, m2, m3 = fac_a1.shape[0], fac_a2.shape[0], fac_a3.shape[0]
        x3 = x_blk.reshape(na, nb, nc)
        d_t = jnp.transpose(diag_blk, (1, 2, 0))
        n_chunk = nb // n_m // CHUNK
        ib, jb = m1 // (n_m * n_x), m2 // n_y
        im = m1 // n_m
        dj, dk, _ = d_t.shape
        n_row = n_m * n_x - 1
        vm = pltpu.VMEM
        dma = pltpu.SemaphoreType.DMA
        pack = nc // dk
        scratch = [
            vm(fac_a1.shape, BF16),
            vm(fac_a2.shape, BF16),
            vm(fac_a3.shape, BF16),
            vm(d_t.shape, F32),
            vm(fac_b2.shape, BF16),
            vm(fac_b3.shape, BF16),
            vm((n_chunk, n_m, na, CHUNK, nc), BF16),
            vm((CHUNK, n_m * na, nc), BF16),
            vm((CHUNK, m1, nc), F32),
            vm((n_chunk, m1, CHUNK, nc), BF16),
            vm((n_m * n_x, n_chunk, ib, CHUNK, nc), BF16),
            vm((ib, m2, nc), BF16),
            vm((n_y, ib, jb, nc), BF16),
            vm((groups, n_x, ib // groups, dj // pack, dk * pack), F32),
            vm((n_x, groups, ib // groups, dj // pack, dk * pack), F32),
            vm((n_y, groups, ib // groups, dj // pack, dk * pack), F32),
            vm((ib, dj, dk * n_y), F32),
            vm((n_x, ib, m2, m3), BF16),
            vm((im // groups, nb, nc), F32),
            dma((6,)),
            dma((n_chunk,)),
            dma((2, n_chunk)),
            dma((2, n_x - 1)),
            dma((2, n_y - 1)),
            dma((2, n_chunk, groups, n_row)),
            dma((2, groups, n_y - 1)),
            dma((2, groups, 2, max(n_x, n_y) - 1)),
            dma((2, groups, 2, max(n_x, n_y) - 1)),
            dma((2, groups)),
        ]
        hbm = pl.BlockSpec(memory_space=pl.ANY)
        v2 = pl.pallas_call(
            functools.partial(core_kernel, (n_m, n_x, n_y, groups)),
            out_shape=jax.ShapeDtypeStruct((nb, m1, nc), BF16),
            in_specs=[pl.BlockSpec(memory_space=pltpu.HBM)] * 7,
            out_specs=pl.BlockSpec(memory_space=pltpu.VMEM),
            scratch_shapes=scratch,
            compiler_params=pltpu.CompilerParams(
                collective_id=0, has_side_effects=True, vmem_limit_bytes=36 * 1024 * 1024),
            name="compress_expand",
        )(*[pltpu.with_memory_space_constraint(v, pltpu.HBM) for v in (x3, fac_a1, fac_a2, fac_a3, d_t, fac_b2, fac_b3)])
        jblk = 32
        z = pl.pallas_call(
            last_kernel,
            out_shape=jax.ShapeDtypeStruct((na, nb, 1, nc), F32),
            grid=(nb // jblk,),
            in_specs=[pl.BlockSpec(fac_b1.shape, lambda j: (0, 0)),
                      pl.BlockSpec((jblk, m1, nc), lambda j: (j, 0, 0))],
            out_specs=hbm,
            scratch_shapes=[vm((2, jblk, na, nc), F32), dma((2,))],
            compiler_params=pltpu.CompilerParams(vmem_limit_bytes=16 * 1024 * 1024),
            name="last_mode",
        )(fac_b1, v2)
        return z.reshape(na, nb, nc, 1)

    return jax.shard_map(
        local_operator, mesh=mesh,
        in_specs=(vol_spec, full_spec, full_spec, full_spec, core_spec, full_spec, full_spec, full_spec),
        out_specs=vol_spec, check_vma=False)
```

```python
import functools

import jax
import jax.numpy as jnp
from jax import lax
from jax.experimental import pallas as pl
from jax.experimental.pallas import tpu as pltpu
from jax.sharding import PartitionSpec as P

MESH = pl.DeviceIdType.MESH
F32 = jnp.float32
BF16 = jnp.bfloat16
CHUNK = 16
NT = (((1,), (1,)), ((), ()))
ORDER = (
    "C0", "S01", "S02", "C1", "S13", "S11", "S12", "C2", "C3", "S31", "S21", "T", "S03", "S33", "S32", "S22",
    "M1", "S23", "D", "S10", "W1", "S00", "M2", "S30", "M3", "S20", "P11", "W2", "P10", "W3", "M0", "P21",
    "P20", "W0", "P30", "P31", "P00", "P01", "E2", "E3", "E1", "E0",
)
FIRST_Y = (2, 2, 2, 2)


def core_kernel(sizes, x_hbm, a1_hbm, a2_hbm, a3_hbm, d_hbm, b2_hbm, b3_hbm, v2_ref,
                a1_ref, a2_ref, a3_ref, d_ref, b2_ref, b3_ref,
                xb, xs, uf, u1, u1r, u2, u2r, dsend, dmid, drecv, dfull, wg, vf,
                sem_f, sem_lx, sem_x, sem_d1, sem_d2, sem_u1, sem_u2, sem_w0, sem_w1, sem_v):
    n_m, n_x, n_y, groups = sizes
    m, xx, yy = lax.axis_index("mx"), lax.axis_index("my"), lax.axis_index("mz")
    rows_a = x_hbm.shape[0]
    half = x_hbm.shape[1] // n_m
    n_chunk = half // CHUNK
    m1 = a1_ref.shape[0]
    ib = m1 // (n_m * n_x)
    ig = ib // groups
    jb = u2r.shape[2]
    im = ib * n_x

    def shift(dm=0, dx=0, dy=0):
        return {"mx": lax.rem(m + dm, n_m), "my": lax.rem(xx + dx, n_x), "mz": lax.rem(yy + dy, n_y)}

    def remote(src, dst, sems, idx, dev):
        cp = pltpu.make_async_remote_copy(
            src_ref=src, dst_ref=dst, send_sem=sems.at[(0,) + idx], recv_sem=sems.at[(1,) + idx],
            device_id=dev, device_id_type=MESH)
        cp.start()
        sent.append(cp)
        return cp

    def local(src, dst, sem):
        cp = pltpu.make_async_copy(src, dst, sem)
        cp.start()
        return cp

    sent = []
    far_x = sorted(range(1, n_x), key=lambda d: (min(d, n_x - d), d))
    far_y = sorted(range(1, n_y), key=lambda d: (min(d, n_y - d), d))
    row = [(dm, dx) for dm in range(n_m) for dx in far_x] + [(dm, 0) for dm in range(1, n_m)]

    barrier = pltpu.get_barrier_semaphore()
    for dm, dx in row:
        pl.semaphore_signal(barrier, inc=1, device_id=shift(dm, dx), device_id_type=MESH)
    for dy in range(1, n_y):
        pl.semaphore_signal(barrier, inc=1, device_id=shift(dy=dy), device_id_type=MESH)
    fac = [local(src, dst, sem_f.at[n]) for n, (src, dst) in enumerate(
        [(d_hbm, d_ref), (a1_hbm, a1_ref), (a2_hbm, a2_ref), (a3_hbm, a3_ref), (b2_hbm, b2_ref), (b3_hbm, b3_ref)])]
    loads = [local(x_hbm.at[:, pl.ds(m * half + q * CHUNK, CHUNK), :], xb.at[q, m], sem_lx.at[q])
             for q in range(n_chunk)]

    def swap_in(q, s):
        @pl.loop(0, rows_a // 128)
        def _(c):
            v = xb[q, s, pl.ds(pl.multiple_of(c * 128, 128), 128)].astype(F32)
            at = pl.multiple_of(s * rows_a + c * 128, 128)
            xs[q, :, pl.ds(at, 128), :] = jnp.swapaxes(v, 0, 1).astype(BF16)

    with jax.named_scope("barrier"):
        pl.semaphore_wait(barrier, len(row) + n_y - 1)

    x_cp = []

    def send_x(q):
        x_cp.append(remote(x_hbm.at[:, pl.ds((1 - m) * half + q * CHUNK, CHUNK), :], xb.at[q, m],
                           sem_x, (q,), shift(dm=1)))

    for q in range(n_chunk):
        send_x(q)
    dk = d_ref.shape[1]
    pack = dsend.shape[4] // dk
    nq = dsend.shape[3]
    with jax.named_scope("d_prep"):
        fac[0].wait()
        parts = [jnp.swapaxes(d_ref[pl.ds(p * nq, nq)], 1, 2) for p in range(pack)]
        packed = jnp.swapaxes(jnp.concatenate(parts, axis=2), 0, 1)
        dsend[...] = packed.reshape(dsend.shape)
        dmid[xx] = dsend[:, xx]
    d1_cp = []
    for dx in range(1, n_x):
        to = lax.rem(xx + dx, n_x)
        d1_cp.append(remote(dsend.at[:, to], dmid.at[xx], sem_d1, (dx - 1,), shift(dx=dx)))
    with jax.named_scope("swap_own"):
        for q in range(4):
            loads[q].wait()
            swap_in(q, m)
    d2_cp = []

    me = xx * n_m + m
    u1_cp = [[] for _ in range(groups)]

    def send_u1(q, g):
        for r, (dm, dx) in enumerate(row):
            base = lax.rem(m + dm, n_m) * im + g * ig * n_x + lax.rem(xx + dx, n_x) * ig
            u1_cp[g].append(remote(u1.at[q, pl.ds(base, ig)], u1r.at[me, q, pl.ds(g * ig, ig)],
                                   sem_u1, (q, g, r), shift(dm, dx)))

    def mode1(q):
        with jax.named_scope("x_wait"):
            x_cp[q].wait_recv()
        with jax.named_scope("swap_in"):
            swap_in(q, 1 - m)
        for cp in fac[1:] if q == 0 else []:
            cp.wait()
        with jax.named_scope("dot1"):
            @pl.loop(0, CHUNK // 2, unroll=8)
            def _(b):
                rhs = jnp.concatenate([xs[q, 2 * b], xs[q, 2 * b + 1]], axis=1)
                out = jnp.dot(a1_ref[...], rhs, preferred_element_type=F32)
                lanes = out.shape[1] // 2
                uf[2 * b] = out[:, :lanes]
                uf[2 * b + 1] = out[:, lanes:]
        with jax.named_scope("swap_out"):
            step = m1 // 4

            @pl.loop(0, 4)
            def _(c):
                v = uf[:, pl.ds(pl.multiple_of(c * step, step), step), :]
                u1[q, pl.ds(c * step, step)] = jnp.swapaxes(v, 0, 1).astype(BF16)
        for g in range(groups):
            u1r[me, q, pl.ds(g * ig, ig)] = u1[q, pl.ds(m * im + g * ig * n_x + xx * ig, ig)]

    u2_cp = [[] for _ in range(groups)]

    def mode2(g):
        with jax.named_scope("u1_wait"):
            for cp in u1_cp[g]:
                cp.wait_recv()
        with jax.named_scope("dot2"):
            @pl.loop(0, ig // 2, unroll=2)
            def _(t):
                i = g * ig + 2 * t
                parts = [u1r[:, :, i + h].reshape(-1, u1r.shape[-1]) for h in range(2)]
                out = jnp.dot(a2_ref[...], jnp.concatenate(parts, axis=1), preferred_element_type=F32)
                lanes = out.shape[1] // 2
                u2[i] = out[:, :lanes].astype(BF16)
                u2[i + 1] = out[:, lanes:].astype(BF16)

        isl = pl.ds(g * ig, ig)
        for dy in far_y:
            to = lax.rem(yy + dy, n_y)
            u2_cp[g].append(remote(u2.at[isl, pl.ds(to * jb, jb), :], u2r.at[yy, isl],
                                   sem_u2, (g, dy - 1), shift(dy=dy)))
        u2r[yy, isl] = u2[isl, pl.ds(pl.multiple_of(yy * jb, jb), jb), :]

    jy = pl.ds(pl.multiple_of(yy * jb, jb), jb)
    w0 = [([], []) for _ in range(groups)]
    w1 = [([], []) for _ in range(groups)]

    def mode3(g):
        with jax.named_scope("u2_wait"):
            for cp in u2_cp[g]:
                cp.wait_recv()
        with jax.named_scope("dot3"):
            isl = pl.ds(g * ig, ig)
            parts = [u2r[s, isl].reshape(ig * jb, -1) for s in range(n_y)]
            out = lax.dot_general(jnp.concatenate(parts, axis=1), a3_ref[...], NT, preferred_element_type=F32)
            u3 = out.astype(BF16).astype(F32).reshape(ig, jb, -1)
            wg[xx, isl, jy, :] = (dfull[isl] * u3).astype(BF16)
        n = FIRST_Y[g]
        for dy in far_y if n else []:
            ref = wg.at[xx, pl.ds(g * ig, n), jy, :]
            w0[g][0].append(remote(ref, ref, sem_w0, (g, 0, dy - 1), shift(dy=dy)))
        for dx in far_x if n < ig else []:
            ref = wg.at[xx, pl.ds(g * ig + n, ig - n), jy, :]
            w1[g][0].append(remote(ref, ref, sem_w1, (g, 0, dx - 1), shift(dx=dx)))

    def gather2(g, k):
        with jax.named_scope(f"p_wait{k}_{g}"):
            for cp in (w0, w1)[k][g][0]:
                cp.wait_recv()
        if k == 0:
            ref = wg.at[xx, pl.ds(g * ig, FIRST_Y[g])]
            for dx in far_x:
                w0[g][1].append(remote(ref, ref, sem_w0, (g, 1, dx - 1), shift(dx=dx)))
        else:
            ref = wg.at[:, pl.ds(g * ig + FIRST_Y[g], ig - FIRST_Y[g]), jy, :]
            for dy in far_y:
                w1[g][1].append(remote(ref, ref, sem_w1, (g, 1, dy - 1), shift(dy=dy)))

    v_cp = []

    def expand(g):
        with jax.named_scope("w_wait3"):
            for cp in w0[g][1] + w1[g][1]:
                cp.wait_recv()
        with jax.named_scope("expand"):
            b3 = b3_ref[pl.ds(pl.multiple_of(yy * b3_ref.shape[1], 128), v2_ref.shape[2]), :]
            b2 = b2_ref[pl.ds(pl.multiple_of(xx * b2_ref.shape[1], 128), v2_ref.shape[0]), :]
            pairs = ig // 2

            @pl.loop(0, n_x * pairs, unroll=8)
            def _(t):
                s = lax.div(t, pairs)
                i = g * ig + 2 * lax.rem(t, pairs)
                w = wg[s, pl.ds(i, 2)].reshape(2 * wg.shape[2], -1)
                v3 = lax.dot_general(w, b3, NT, preferred_element_type=F32).astype(BF16)
                rows = v3.shape[0] // 2
                rhs = jnp.concatenate([v3[:rows], v3[rows:]], axis=1)
                out = jnp.dot(b2, rhs, preferred_element_type=F32)
                lanes = out.shape[1] // 2
                vf[2 * t] = out[:, :lanes]
                vf[2 * t + 1] = out[:, lanes:]

        mine = pl.multiple_of(m * im + g * ig * n_x, ig * n_x)
        step = vf.shape[1] // 4
        with jax.named_scope("swap_v"):
            @pl.loop(0, 4)
            def _(c):
                at = pl.multiple_of(c * step, step)
                v2_ref[pl.ds(at, step), pl.ds(mine, ig * n_x), :] = jnp.swapaxes(
                    vf[:, pl.ds(at, step), :], 0, 1).astype(BF16)
        ref = v2_ref.at[:, pl.ds(mine, ig * n_x), :]
        v_cp.append(remote(ref, ref, sem_v, (g,), shift(dm=1)))

    def diag_turn():
        with jax.named_scope("d1_wait"):
            for cp in d1_cp:
                cp.wait_recv()
        for dy in range(1, n_y):
            to = lax.rem(yy + dy, n_y)
            d2_cp.append(remote(dmid.at[to], drecv.at[yy], sem_d2, (dy - 1,), shift(dy=dy)))
        drecv[yy] = dmid[yy]

    def diag_full():
        with jax.named_scope("d_full"):
            for cp in d2_cp:
                cp.wait_recv()
            lanes = [drecv[s].reshape(ib, nq, -1) for s in range(n_y)]
            parts = [jnp.concatenate([v[:, :, p * dk:(p + 1) * dk] for v in lanes], axis=2) for p in range(pack)]
            dfull[...] = jnp.concatenate(parts, axis=1)

    steps = {"C": mode1, "S": send_u1, "T": diag_turn, "D": diag_full, "M": mode2, "W": mode3,
             "P": gather2, "E": expand}
    for word in ORDER:
        steps[word[0]](*[int(c) for c in word[1:]])
    with jax.named_scope("v_wait"):
        for cp in v_cp:
            cp.wait_recv()
    for cp in sent:
        cp.wait_send()


def last_kernel(b1_ref, v_ref, z_hbm, buf, sem):
    rows = buf.shape[2]
    s, n = pl.program_id(0), pl.num_programs(0)
    slot = lax.rem(s, 2)
    width = v_ref.shape[0]

    def drain(k):
        pltpu.make_async_copy(buf.at[k], buf.at[k], sem.at[k]).wait()

    @pl.when(s >= 2)
    def _():
        drain(slot)

    b1 = b1_ref[pl.ds(pl.multiple_of(lax.axis_index("mx") * rows, rows), rows), :]
    for q in range(0, width, 2):
        rhs = jnp.concatenate([v_ref[q], v_ref[q + 1]], axis=1)
        out = jnp.dot(b1, rhs, preferred_element_type=F32)
        lanes = out.shape[1] // 2
        for h in range(2):
            buf[slot, q + h] = out[:, h * lanes:(h + 1) * lanes]
            pltpu.make_async_copy(buf.at[slot, q + h], z_hbm.at[:, s * width + q + h, 0, :], sem.at[slot]).start()

    @pl.when(s == n - 1)
    def _():
        drain(0)
        drain(1)


def solution(mesh):
    vol_spec = P("mx", "my", "mz", "rhs")
    core_spec = P("mx", "my", "mz")
    full_spec = P()
    n_m, n_x, n_y = mesh.shape["mx"], mesh.shape["my"], mesh.shape["mz"]
    groups = 4

    def local_operator(x_blk, fac_a1, fac_a2, fac_a3, diag_blk, fac_b1, fac_b2, fac_b3):
        na, nb, nc = x_blk.shape[:3]
        m1, m2, m3 = fac_a1.shape[0], fac_a2.shape[0], fac_a3.shape[0]
        x3 = x_blk.reshape(na, nb, nc)
        d_t = jnp.transpose(diag_blk, (1, 2, 0))
        n_chunk = nb // n_m // CHUNK
        ib, jb = m1 // (n_m * n_x), m2 // n_y
        im = m1 // n_m
        dj, dk, _ = d_t.shape
        n_row = n_m * n_x - 1
        vm = pltpu.VMEM
        dma = pltpu.SemaphoreType.DMA
        pack = nc // dk
        scratch = [
            vm(fac_a1.shape, BF16),
            vm(fac_a2.shape, BF16),
            vm(fac_a3.shape, BF16),
            vm(d_t.shape, F32),
            vm(fac_b2.shape, BF16),
            vm(fac_b3.shape, BF16),
            vm((n_chunk, n_m, na, CHUNK, nc), BF16),
            vm((n_chunk, CHUNK, n_m * na, nc), BF16),
            vm((CHUNK, m1, nc), F32),
            vm((n_chunk, m1, CHUNK, nc), BF16),
            vm((n_m * n_x, n_chunk, ib, CHUNK, nc), BF16),
            vm((ib, m2, nc), BF16),
            vm((n_y, ib, jb, nc), BF16),
            vm((groups, n_x, ib // groups, dj // pack, dk * pack), F32),
            vm((n_x, groups, ib // groups, dj // pack, dk * pack), F32),
            vm((n_y, groups, ib // groups, dj // pack, dk * pack), F32),
            vm((ib, dj, dk * n_y), F32),
            vm((n_x, ib, m2, m3), BF16),
            vm((im // groups, nb, nc), F32),
            dma((6,)),
            dma((n_chunk,)),
            dma((2, n_chunk)),
            dma((2, n_x - 1)),
            dma((2, n_y - 1)),
            dma((2, n_chunk, groups, n_row)),
            dma((2, groups, n_y - 1)),
            dma((2, groups, 2, max(n_x, n_y) - 1)),
            dma((2, groups, 2, max(n_x, n_y) - 1)),
            dma((2, groups)),
        ]
        hbm = pl.BlockSpec(memory_space=pl.ANY)
        v2 = pl.pallas_call(
            functools.partial(core_kernel, (n_m, n_x, n_y, groups)),
            out_shape=jax.ShapeDtypeStruct((nb, m1, nc), BF16),
            in_specs=[pl.BlockSpec(memory_space=pltpu.HBM)] * 7,
            out_specs=pl.BlockSpec(memory_space=pltpu.VMEM),
            scratch_shapes=scratch,
            compiler_params=pltpu.CompilerParams(
                collective_id=0, has_side_effects=True, vmem_limit_bytes=36 * 1024 * 1024),
            name="compress_expand",
        )(*[pltpu.with_memory_space_constraint(v, pltpu.HBM) for v in (x3, fac_a1, fac_a2, fac_a3, d_t, fac_b2, fac_b3)])
        jblk = 32
        z = pl.pallas_call(
            last_kernel,
            out_shape=jax.ShapeDtypeStruct((na, nb, 1, nc), F32),
            grid=(nb // jblk,),
            in_specs=[pl.BlockSpec(fac_b1.shape, lambda j: (0, 0)),
                      pl.BlockSpec((jblk, m1, nc), lambda j: (j, 0, 0))],
            out_specs=hbm,
            scratch_shapes=[vm((2, jblk, na, nc), F32), dma((2,))],
            compiler_params=pltpu.CompilerParams(vmem_limit_bytes=16 * 1024 * 1024),
            name="last_mode",
        )(fac_b1, v2)
        return z.reshape(na, nb, nc, 1)

    return jax.shard_map(
        local_operator, mesh=mesh,
        in_specs=(vol_spec, full_spec, full_spec, full_spec, core_spec, full_spec, full_spec, full_spec),
        out_specs=vol_spec, check_vma=False)
```

```python
import functools

import jax
import jax.numpy as jnp
from jax import lax
from jax.experimental import pallas as pl
from jax.experimental.pallas import tpu as pltpu
from jax.sharding import PartitionSpec as P

MESH = pl.DeviceIdType.MESH
F32 = jnp.float32
BF16 = jnp.bfloat16
CHUNK = 16
NT = (((1,), (1,)), ((), ()))
ORDER = (
    "C0", "S01", "S02", "C1", "S13", "S11", "S12", "C2", "C3", "S31", "S21", "T", "S03", "S33", "S32", "S22",
    "M1", "S23", "D", "S10", "W1", "S00", "M2", "S30", "M3", "S20", "P11", "W2", "P10", "W3", "M0", "P21",
    "P20", "W0", "P30", "P31", "P00", "P01", "E2", "E3", "E1", "E0",
)
FIRST_Y = (2, 2, 2, 2)


def core_kernel(sizes, x_hbm, a1_hbm, a2_hbm, a3_hbm, d_hbm, b2_hbm, b3_hbm, v2_ref,
                a1_ref, a2_ref, a3_ref, d_ref, b2_ref, b3_ref,
                xb, xs, uf, u1, u1r, u2, u2r, dsend, dmid, drecv, dfull, wg, vf,
                sem_f, sem_lx, sem_x, sem_d1, sem_d2, sem_u1, sem_us, sem_u2, sem_w0, sem_w1, sem_v):
    n_m, n_x, n_y, groups = sizes
    m, xx, yy = lax.axis_index("mx"), lax.axis_index("my"), lax.axis_index("mz")
    rows_a = x_hbm.shape[0]
    half = x_hbm.shape[1] // n_m
    n_chunk = half // CHUNK
    m1 = a1_ref.shape[0]
    ib = m1 // (n_m * n_x)
    ig = ib // groups
    jb = u2r.shape[2]
    im = ib * n_x

    def shift(dm=0, dx=0, dy=0):
        return {"mx": lax.rem(m + dm, n_m), "my": lax.rem(xx + dx, n_x), "mz": lax.rem(yy + dy, n_y)}

    def remote(src, dst, sems, idx, dev):
        cp = pltpu.make_async_remote_copy(
            src_ref=src, dst_ref=dst, send_sem=sems.at[(0,) + idx], recv_sem=sems.at[(1,) + idx],
            device_id=dev, device_id_type=MESH)
        cp.start()
        sent.append(cp)
        return cp

    def local(src, dst, sem):
        cp = pltpu.make_async_copy(src, dst, sem)
        cp.start()
        return cp

    sent = []
    far_x = sorted(range(1, n_x), key=lambda d: (min(d, n_x - d), d))
    far_y = sorted(range(1, n_y), key=lambda d: (min(d, n_y - d), d))
    row = [(dm, dx) for dm in range(n_m) for dx in far_x] + [(dm, 0) for dm in range(1, n_m)]

    barrier = pltpu.get_barrier_semaphore()
    for dm, dx in row:
        pl.semaphore_signal(barrier, inc=1, device_id=shift(dm, dx), device_id_type=MESH)
    for dy in range(1, n_y):
        pl.semaphore_signal(barrier, inc=1, device_id=shift(dy=dy), device_id_type=MESH)
    fac = [local(src, dst, sem_f.at[n]) for n, (src, dst) in enumerate(
        [(d_hbm, d_ref), (a1_hbm, a1_ref), (a2_hbm, a2_ref), (a3_hbm, a3_ref), (b2_hbm, b2_ref), (b3_hbm, b3_ref)])]
    loads = [local(x_hbm.at[:, pl.ds(m * half + q * CHUNK, CHUNK), :], xb.at[q, m], sem_lx.at[q])
             for q in range(n_chunk)]

    def swap_in(q, s):
        @pl.loop(0, rows_a // 128)
        def _(c):
            v = xb[q, s, pl.ds(pl.multiple_of(c * 128, 128), 128)].astype(F32)
            at = pl.multiple_of(s * rows_a + c * 128, 128)
            xs[q, :, pl.ds(at, 128), :] = jnp.swapaxes(v, 0, 1).astype(BF16)

    with jax.named_scope("barrier"):
        pl.semaphore_wait(barrier, len(row) + n_y - 1)

    x_cp = []

    def send_x(q):
        x_cp.append(remote(x_hbm.at[:, pl.ds((1 - m) * half + q * CHUNK, CHUNK), :], xb.at[q, m],
                           sem_x, (q,), shift(dm=1)))

    for q in range(n_chunk):
        send_x(q)
    dk = d_ref.shape[1]
    pack = dsend.shape[4] // dk
    nq = dsend.shape[3]
    with jax.named_scope("d_prep"):
        fac[0].wait()
        parts = [jnp.swapaxes(d_ref[pl.ds(p * nq, nq)], 1, 2) for p in range(pack)]
        packed = jnp.swapaxes(jnp.concatenate(parts, axis=2), 0, 1)
        dsend[...] = packed.reshape(dsend.shape)
        dmid[xx] = dsend[:, xx]
    d1_cp = []
    for dx in range(1, n_x):
        to = lax.rem(xx + dx, n_x)
        d1_cp.append(remote(dsend.at[:, to], dmid.at[xx], sem_d1, (dx - 1,), shift(dx=dx)))
    with jax.named_scope("swap_own"):
        for q in range(4):
            loads[q].wait()
            swap_in(q, m)
    d2_cp = []

    me = xx * n_m + m
    u1_cp = [[] for _ in range(groups)]

    def send_u1(q, g):
        for r, (dm, dx) in enumerate(row):
            base = lax.rem(m + dm, n_m) * im + g * ig * n_x + lax.rem(xx + dx, n_x) * ig
            cp = pltpu.make_async_remote_copy(
                src_ref=u1.at[q, pl.ds(base, ig)], dst_ref=u1r.at[me, q, pl.ds(g * ig, ig)],
                send_sem=sem_us, recv_sem=sem_u1.at[q, g, r], device_id=shift(dm, dx), device_id_type=MESH)
            cp.start()
            u1_cp[g].append(cp)

    def mode1(q):
        with jax.named_scope("x_wait"):
            x_cp[q].wait_recv()
        with jax.named_scope("swap_in"):
            swap_in(q, 1 - m)
        for cp in fac[1:] if q == 0 else []:
            cp.wait()
        with jax.named_scope("dot1"):
            @pl.loop(0, CHUNK // 2, unroll=8)
            def _(b):
                rhs = jnp.concatenate([xs[q, 2 * b], xs[q, 2 * b + 1]], axis=1)
                out = jnp.dot(a1_ref[...], rhs, preferred_element_type=F32)
                lanes = out.shape[1] // 2
                uf[2 * b] = out[:, :lanes]
                uf[2 * b + 1] = out[:, lanes:]
        with jax.named_scope("swap_out"):
            step = m1 // 4

            @pl.loop(0, 4)
            def _(c):
                v = uf[:, pl.ds(pl.multiple_of(c * step, step), step), :]
                u1[q, pl.ds(c * step, step)] = jnp.swapaxes(v, 0, 1).astype(BF16)
        for g in range(groups):
            u1r[me, q, pl.ds(g * ig, ig)] = u1[q, pl.ds(m * im + g * ig * n_x + xx * ig, ig)]

    u2_cp = [[] for _ in range(groups)]

    def mode2(g):
        with jax.named_scope("u1_wait"):
            for cp in u1_cp[g]:
                cp.wait_recv()
        with jax.named_scope("dot2"):
            @pl.loop(0, ig // 2, unroll=2)
            def _(t):
                i = g * ig + 2 * t
                parts = [u1r[:, :, i + h].reshape(-1, u1r.shape[-1]) for h in range(2)]
                out = jnp.dot(a2_ref[...], jnp.concatenate(parts, axis=1), preferred_element_type=F32)
                lanes = out.shape[1] // 2
                u2[i] = out[:, :lanes].astype(BF16)
                u2[i + 1] = out[:, lanes:].astype(BF16)

        isl = pl.ds(g * ig, ig)
        for dy in far_y:
            to = lax.rem(yy + dy, n_y)
            u2_cp[g].append(remote(u2.at[isl, pl.ds(to * jb, jb), :], u2r.at[yy, isl],
                                   sem_u2, (g, dy - 1), shift(dy=dy)))
        u2r[yy, isl] = u2[isl, pl.ds(pl.multiple_of(yy * jb, jb), jb), :]

    jy = pl.ds(pl.multiple_of(yy * jb, jb), jb)
    w0 = [([], []) for _ in range(groups)]
    w1 = [([], []) for _ in range(groups)]

    def mode3(g):
        with jax.named_scope("u2_wait"):
            for cp in u2_cp[g]:
                cp.wait_recv()
        with jax.named_scope("dot3"):
            isl = pl.ds(g * ig, ig)
            parts = [u2r[s, isl].reshape(ig * jb, -1) for s in range(n_y)]
            out = lax.dot_general(jnp.concatenate(parts, axis=1), a3_ref[...], NT, preferred_element_type=F32)
            u3 = out.astype(BF16).astype(F32).reshape(ig, jb, -1)
            wg[xx, isl, jy, :] = (dfull[isl] * u3).astype(BF16)
        n = FIRST_Y[g]
        for dy in far_y if n else []:
            ref = wg.at[xx, pl.ds(g * ig, n), jy, :]
            w0[g][0].append(remote(ref, ref, sem_w0, (g, 0, dy - 1), shift(dy=dy)))
        for dx in far_x if n < ig else []:
            ref = wg.at[xx, pl.ds(g * ig + n, ig - n), jy, :]
            w1[g][0].append(remote(ref, ref, sem_w1, (g, 0, dx - 1), shift(dx=dx)))

    def gather2(g, k):
        with jax.named_scope(f"p_wait{k}_{g}"):
            for cp in (w0, w1)[k][g][0]:
                cp.wait_recv()
        if k == 0:
            ref = wg.at[xx, pl.ds(g * ig, FIRST_Y[g])]
            for dx in far_x:
                w0[g][1].append(remote(ref, ref, sem_w0, (g, 1, dx - 1), shift(dx=dx)))
        else:
            ref = wg.at[:, pl.ds(g * ig + FIRST_Y[g], ig - FIRST_Y[g]), jy, :]
            for dy in far_y:
                w1[g][1].append(remote(ref, ref, sem_w1, (g, 1, dy - 1), shift(dy=dy)))

    v_cp = []

    def expand(g):
        with jax.named_scope("w_wait3"):
            for cp in w0[g][1] + w1[g][1]:
                cp.wait_recv()
        with jax.named_scope("expand"):
            b3 = b3_ref[pl.ds(pl.multiple_of(yy * b3_ref.shape[1], 128), v2_ref.shape[2]), :]
            b2 = b2_ref[pl.ds(pl.multiple_of(xx * b2_ref.shape[1], 128), v2_ref.shape[0]), :]
            pairs = ig // 2

            @pl.loop(0, n_x * pairs, unroll=8)
            def _(t):
                s = lax.div(t, pairs)
                i = g * ig + 2 * lax.rem(t, pairs)
                w = wg[s, pl.ds(i, 2)].reshape(2 * wg.shape[2], -1)
                v3 = lax.dot_general(w, b3, NT, preferred_element_type=F32).astype(BF16)
                rows = v3.shape[0] // 2
                rhs = jnp.concatenate([v3[:rows], v3[rows:]], axis=1)
                out = jnp.dot(b2, rhs, preferred_element_type=F32)
                lanes = out.shape[1] // 2
                vf[2 * t] = out[:, :lanes]
                vf[2 * t + 1] = out[:, lanes:]

        mine = pl.multiple_of(m * im + g * ig * n_x, ig * n_x)
        step = vf.shape[1] // 4
        with jax.named_scope("swap_v"):
            @pl.loop(0, 4)
            def _(c):
                at = pl.multiple_of(c * step, step)
                v2_ref[pl.ds(at, step), pl.ds(mine, ig * n_x), :] = jnp.swapaxes(
                    vf[:, pl.ds(at, step), :], 0, 1).astype(BF16)
        ref = v2_ref.at[:, pl.ds(mine, ig * n_x), :]
        v_cp.append(remote(ref, ref, sem_v, (g,), shift(dm=1)))

    def diag_turn():
        with jax.named_scope("d1_wait"):
            for cp in d1_cp:
                cp.wait_recv()
        for dy in range(1, n_y):
            to = lax.rem(yy + dy, n_y)
            d2_cp.append(remote(dmid.at[to], drecv.at[yy], sem_d2, (dy - 1,), shift(dy=dy)))
        drecv[yy] = dmid[yy]

    def diag_full():
        with jax.named_scope("d_full"):
            for cp in d2_cp:
                cp.wait_recv()
            lanes = [drecv[s].reshape(ib, nq, -1) for s in range(n_y)]
            parts = [jnp.concatenate([v[:, :, p * dk:(p + 1) * dk] for v in lanes], axis=2) for p in range(pack)]
            dfull[...] = jnp.concatenate(parts, axis=1)

    steps = {"C": mode1, "S": send_u1, "T": diag_turn, "D": diag_full, "M": mode2, "W": mode3,
             "P": gather2, "E": expand}
    drained = []

    def drain(copies):
        for cp in copies:
            if not any(cp is old for old in drained):
                cp.wait_send()
                drained.append(cp)

    final = {word[0]: n for n, word in enumerate(ORDER)}
    for n, word in enumerate(ORDER):
        if n == final["W"]:
            drain(x_cp + d1_cp + d2_cp)
            peers = u1r.at[pl.ds(0, len(row))]
            pltpu.make_async_copy(peers, peers, sem_us).wait()
        if n == final["P"]:
            drain(sum(u2_cp, []) + sum([a for a, _ in w0 + w1], []))
        if n == final["E"]:
            drain(sum([b for _, b in w0 + w1], []))
        steps[word[0]](*[int(c) for c in word[1:]])
    with jax.named_scope("v_wait"):
        for cp in v_cp:
            cp.wait_recv()
    drain(sent)


def last_kernel(b1_ref, v_ref, z_hbm, buf, sem):
    rows = buf.shape[2]
    s, n = pl.program_id(0), pl.num_programs(0)
    slot = lax.rem(s, 2)
    width = v_ref.shape[0]

    def drain(k):
        pltpu.make_async_copy(buf.at[k], buf.at[k], sem.at[k]).wait()

    @pl.when(s >= 2)
    def _():
        drain(slot)

    b1 = b1_ref[pl.ds(pl.multiple_of(lax.axis_index("mx") * rows, rows), rows), :]
    for q in range(0, width, 2):
        rhs = jnp.concatenate([v_ref[q], v_ref[q + 1]], axis=1)
        out = jnp.dot(b1, rhs, preferred_element_type=F32)
        lanes = out.shape[1] // 2
        for h in range(2):
            buf[slot, q + h] = out[:, h * lanes:(h + 1) * lanes]
            pltpu.make_async_copy(buf.at[slot, q + h], z_hbm.at[:, s * width + q + h, 0, :], sem.at[slot]).start()

    @pl.when(s == n - 1)
    def _():
        drain(0)
        drain(1)


def solution(mesh):
    vol_spec = P("mx", "my", "mz", "rhs")
    core_spec = P("mx", "my", "mz")
    full_spec = P()
    n_m, n_x, n_y = mesh.shape["mx"], mesh.shape["my"], mesh.shape["mz"]
    groups = 4

    def local_operator(x_blk, fac_a1, fac_a2, fac_a3, diag_blk, fac_b1, fac_b2, fac_b3):
        na, nb, nc = x_blk.shape[:3]
        m1, m2, m3 = fac_a1.shape[0], fac_a2.shape[0], fac_a3.shape[0]
        x3 = x_blk.reshape(na, nb, nc)
        d_t = jnp.transpose(diag_blk, (1, 2, 0))
        n_chunk = nb // n_m // CHUNK
        ib, jb = m1 // (n_m * n_x), m2 // n_y
        im = m1 // n_m
        dj, dk, _ = d_t.shape
        n_row = n_m * n_x - 1
        vm = pltpu.VMEM
        dma = pltpu.SemaphoreType.DMA
        pack = nc // dk
        scratch = [
            vm(fac_a1.shape, BF16),
            vm(fac_a2.shape, BF16),
            vm(fac_a3.shape, BF16),
            vm(d_t.shape, F32),
            vm(fac_b2.shape, BF16),
            vm(fac_b3.shape, BF16),
            vm((n_chunk, n_m, na, CHUNK, nc), BF16),
            vm((n_chunk, CHUNK, n_m * na, nc), BF16),
            vm((CHUNK, m1, nc), F32),
            vm((n_chunk, m1, CHUNK, nc), BF16),
            vm((n_m * n_x, n_chunk, ib, CHUNK, nc), BF16),
            vm((ib, m2, nc), BF16),
            vm((n_y, ib, jb, nc), BF16),
            vm((groups, n_x, ib // groups, dj // pack, dk * pack), F32),
            vm((n_x, groups, ib // groups, dj // pack, dk * pack), F32),
            vm((n_y, groups, ib // groups, dj // pack, dk * pack), F32),
            vm((ib, dj, dk * n_y), F32),
            vm((n_x, ib, m2, m3), BF16),
            vm((im // groups, nb, nc), F32),
            dma((6,)),
            dma((n_chunk,)),
            dma((2, n_chunk)),
            dma((2, n_x - 1)),
            dma((2, n_y - 1)),
            dma((n_chunk, groups, n_row)),
            dma,
            dma((2, groups, n_y - 1)),
            dma((2, groups, 2, max(n_x, n_y) - 1)),
            dma((2, groups, 2, max(n_x, n_y) - 1)),
            dma((2, groups)),
        ]
        hbm = pl.BlockSpec(memory_space=pl.ANY)
        v2 = pl.pallas_call(
            functools.partial(core_kernel, (n_m, n_x, n_y, groups)),
            out_shape=jax.ShapeDtypeStruct((nb, m1, nc), BF16),
            in_specs=[pl.BlockSpec(memory_space=pltpu.HBM)] * 7,
            out_specs=pl.BlockSpec(memory_space=pltpu.VMEM),
            scratch_shapes=scratch,
            compiler_params=pltpu.CompilerParams(
                collective_id=0, has_side_effects=True, vmem_limit_bytes=36 * 1024 * 1024),
            name="compress_expand",
        )(*[pltpu.with_memory_space_constraint(v, pltpu.HBM) for v in (x3, fac_a1, fac_a2, fac_a3, d_t, fac_b2, fac_b3)])
        jblk = 32
        z = pl.pallas_call(
            last_kernel,
            out_shape=jax.ShapeDtypeStruct((na, nb, 1, nc), F32),
            grid=(nb // jblk,),
            in_specs=[pl.BlockSpec(fac_b1.shape, lambda j: (0, 0)),
                      pl.BlockSpec((jblk, m1, nc), lambda j: (j, 0, 0))],
            out_specs=hbm,
            scratch_shapes=[vm((2, jblk, na, nc), F32), dma((2,))],
            compiler_params=pltpu.CompilerParams(vmem_limit_bytes=16 * 1024 * 1024),
            name="last_mode",
        )(fac_b1, v2)
        return z.reshape(na, nb, nc, 1)

    return jax.shard_map(
        local_operator, mesh=mesh,
        in_specs=(vol_spec, full_spec, full_spec, full_spec, core_spec, full_spec, full_spec, full_spec),
        out_specs=vol_spec, check_vma=False)
```
